32 devices in a mesh: rep: 2 (over x), dp: 16 (over y, z, core).
Axes of the slice: x: 2, y: 2, z: 4, core: 2. Of those that a mesh axis runs over, the one named last changes fastest.
Arguments:
- g_w_gate: bfloat16 [32, 2, 1024, 3072], P(('rep', 'dp')), parts along dimension 0
- g_w_up: bfloat16 [32, 2, 1024, 3072], P(('rep', 'dp')), parts along dimension 0
- g_w_down: bfloat16 [32, 2, 3072, 1024], P(('rep', 'dp')), parts along dimension 0
- w_gate: bfloat16 [2, 1024, 3072], replicated
- w_up: bfloat16 [2, 1024, 3072], replicated
- w_down: bfloat16 [2, 3072, 1024], replicated
- m_w_gate: float32 [2, 1024, 3072], P(None, 'dp')
- m_w_up: float32 [2, 1024, 3072], P(None, 'dp')
- m_w_down: float32 [2, 3072, 1024], P(None, 'dp')
- v_w_gate: float32 [2, 1024, 3072], P(None, 'dp')
- v_w_up: float32 [2, 1024, 3072], P(None, 'dp')
- v_w_down: float32 [2, 3072, 1024], P(None, 'dp')
Outputs:
- output 1: bfloat16 [4, 1024, 3072], P('rep'), parts along dimension 0
- output 2: bfloat16 [4, 1024, 3072], P('rep'), parts along dimension 0
- output 3: bfloat16 [4, 3072, 1024], P('rep'), parts along dimension 0
- output 4: float32 [4, 1024, 3072], P('rep', 'dp'), parts along dimension 0
- output 5: float32 [4, 1024, 3072], P('rep', 'dp'), parts along dimension 0
- output 6: float32 [4, 3072, 1024], P('rep', 'dp'), parts along dimension 0
- output 7: float32 [4, 1024, 3072], P('rep', 'dp'), parts along dimension 0
- output 8: float32 [4, 1024, 3072], P('rep', 'dp'), parts along dimension 0
- output 9: float32 [4, 3072, 1024], P('rep', 'dp'), parts along dimension 0
There are 2 independent parts. The reference program is written for one: setup_inputs(seed, part) draws one part's arguments, and reference() takes and returns one part's arrays. A program takes and returns all parts, laid end to end along the dimension named above; an argument that names none is the same for every part.
All inputs are finite; a program needn't handle non-finite values.
Results may differ from the reference program's by a relative error of at most 0.022.
Values are sent between devices in bfloat16 or wider.
A program may use at most 2 GiB of HBM per device.

```python
import jax
import jax.numpy as jnp
from jax import lax

DEVICES = 16
D = 1024
FF = 3072
LAYERS = 2
NAMES = ("w_gate", "w_up", "w_down")
SHAPES = {"w_gate": (LAYERS, D, FF), "w_up": (LAYERS, D, FF), "w_down": (LAYERS, FF, D)}


def setup_inputs(seed: int = 0, part: int = 0) -> dict:
    kz, *keys = jax.random.split(jax.random.key(seed), 1 + 5 * len(NAMES))
    loud = 2.0 ** jax.random.uniform(kz, (), jnp.float32, -1.0, 1.0)
    drawn = {}
    for name, key, both in zip(NAMES, keys[:3], keys[3:6], strict=True):
        own = jax.random.normal(jax.random.fold_in(key, part), (DEVICES, *SHAPES[name]), jnp.float32)
        shared = jax.random.normal(jax.random.fold_in(both, part), SHAPES[name], jnp.float32)
        drawn["g_" + name] = (loud * (0.7 * shared / DEVICES + 0.7 * own * DEVICES**-0.5)).astype(jnp.bfloat16)
    for name, key in zip(NAMES, keys[6:9], strict=True):
        drawn[name] = (jax.random.normal(key, SHAPES[name], jnp.float32) * SHAPES[name][1] ** -0.5).astype(jnp.bfloat16)
    for name, key in zip(NAMES, keys[9:12], strict=True):
        drawn["m_" + name] = loud * 0.5 * jax.random.normal(key, SHAPES[name], jnp.float32)
    for name, key in zip(NAMES, keys[12:15], strict=True):
        drawn["v_" + name] = loud * loud * jax.random.uniform(key, SHAPES[name], jnp.float32, 0.5, 1.5)
    return drawn


def adamw(w, m, v, g):
    m = 0.9 * m + 0.1 * g
    v = 0.95 * v + 0.05 * g * g
    step = m * lax.rsqrt(v + 1e-8) + 0.1 * w
    return (w - 0.02 * step).astype(jnp.bfloat16), m, v


def reference(g_w_gate, g_w_up, g_w_down, w_gate, w_up, w_down, m_w_gate, m_w_up, m_w_down, v_w_gate, v_w_up, v_w_down):
    def total(terms):
        return lax.scan(lambda so_far, term: (so_far + term.astype(jnp.float32), None), jnp.zeros(terms.shape[1:], jnp.float32), terms)[0]

    gradients = [total(terms).astype(jnp.bfloat16).astype(jnp.float32) for terms in (g_w_gate, g_w_up, g_w_down)]
    new = [
        adamw(w.astype(jnp.float32), m, v, g)
        for w, m, v, g in zip((w_gate, w_up, w_down), (m_w_gate, m_w_up, m_w_down), (v_w_gate, v_w_up, v_w_down), gradients, strict=True)
    ]
    return tuple(one[which] for which in range(3) for one in new)
```

```python
import functools

import jax
import jax.numpy as jnp
from jax import lax
from jax.experimental import pallas as pl
from jax.experimental.pallas import tpu as pltpu
from jax.sharding import PartitionSpec as P

MESH = pl.DeviceIdType.MESH
Y, Z = 2, 4
CUTS = 8
ACC = 9
STAGED = 4
STAGES = 10


def kernel(groups, cuts, acc_slots, *refs):
    terms, weights, moments_m, moments_v = (refs[i : i + 3] for i in (0, 3, 6, 9))
    whole, new_m, new_v = (refs[i : i + 3] for i in (12, 15, 18))
    acc_a, acc_b, all_a, all_b, y_a, y_b, z_a, z_b, w_a, w_b, m_a, m_b, v_a, v_b = refs[21:35]
    load_sem, pair_send, pair_recv, y_send, y_recv, z_send, z_recv, spread_send, spread_recv = refs[35:44]
    back_send, back_recv, out_send, out_recv, store_sem, state_sem, keep_sem = refs[44:51]

    rep, me = lax.axis_index("rep"), lax.axis_index("dp")
    c = lax.rem(me, 2)
    z = lax.rem(me // 2, Z)
    y = me // (2 * Z)
    far = Z - 1 - z
    partner = me + 1 - 2 * c
    across = me + (1 - 2 * y) * (2 * Z)
    beside = (me + 2, me - 2)
    place = (z, far)

    def send_to(device, src, dst, send_sem, recv_sem):
        return pltpu.make_async_remote_copy(
            src_ref=src, dst_ref=dst, send_sem=send_sem, recv_sem=recv_sem, device_id=(rep, device), device_id_type=MESH
        )

    def f32(x):
        return x.astype(jnp.float32)

    def own_load(g, k):
        layer, h, slot = g // cuts, lax.rem(g, cuts), lax.rem(g, acc_slots)
        dst = acc_b.at[slot] if k == 2 else acc_a.at[slot, k]
        return pltpu.make_async_copy(terms[k].at[layer, :, :, c, h], dst, load_sem.at[lax.rem(g, 4), k])

    def pair_copy(g, k):
        layer, h = g // cuts, lax.rem(g, cuts)
        dst = all_b.at[g] if k == 2 else all_a.at[g, k]
        return send_to(partner, terms[k].at[layer, :, :, 1 - c, h], dst, pair_send.at[lax.rem(g, 4), k], pair_recv.at[g, k])

    def y_copy(g, kind):
        slot = lax.rem(g, acc_slots)
        src, dst = (acc_b.at[slot, 1 - y, z], y_b.at[g]) if kind else (acc_a.at[slot, :, 1 - y], y_a.at[g])
        return send_to(across, src, dst, y_send.at[lax.rem(g, 2), kind], y_recv.at[g, kind])

    def z_copy(g, kind, way, s):
        slot = lax.rem(g, acc_slots)
        t = Z - 1 - s + z if way == 0 else s - far
        src, dst = (acc_b.at[slot, :, t], z_b.at[g, way, s]) if kind else (acc_a.at[slot, :, y, t], z_a.at[g, way, s])
        return send_to(beside[way], src, dst, z_send.at[lax.rem(g, 2), kind, way, s], z_recv.at[g, kind, way, s])

    def spread_copy(g, kind, way, s):
        t = z - s if way == 0 else z + s
        ref = all_b.at[g, :, t] if kind else all_a.at[g, :, y, t]
        return send_to(beside[way], ref, ref, spread_send.at[lax.rem(g, 2), kind, way, s], spread_recv.at[g, kind, way, s])

    def back_copy(g, kind):
        ref = all_b.at[g, y, z] if kind else all_a.at[g, :, y]
        return send_to(across, ref, ref, back_send.at[lax.rem(g, 2), kind], back_recv.at[g, kind])

    def out_parts(g, k, half):
        layer, h = g // cuts, lax.rem(g, cuts)
        if k == 2:
            return all_b.at[g], whole[k].at[layer, :, :, c, h], 4
        which = 1 - y if half else y
        return all_a.at[g, k, which], whole[k].at[layer, which, :, c, h], 2 * k + half

    def out_copy(g, k, half):
        src, dst, i = out_parts(g, k, half)
        return send_to(partner, src, dst, out_send.at[lax.rem(g, 2), i], out_recv.at[g, i])

    def out_store(g, k, half):
        src, dst, i = out_parts(g, k, half)
        return pltpu.make_async_copy(src, dst, store_sem.at[lax.rem(g, 2), i])

    def state_loads(g):
        layer, h, slot = g // cuts, lax.rem(g, cuts), lax.rem(g, STAGED)
        copies = []
        for k in range(3):
            w_ref, m_ref, v_ref = (w_b, m_b, v_b) if k == 2 else (w_a, m_a, v_a)
            at = (slot,) if k == 2 else (slot, k)
            copies.append(pltpu.make_async_copy(weights[k].at[layer, y, z, c, h], w_ref.at[at], state_sem.at[slot, 3 * k]))
            copies.append(pltpu.make_async_copy(moments_m[k].at[layer, h], m_ref.at[at], state_sem.at[slot, 3 * k + 1]))
            copies.append(pltpu.make_async_copy(moments_v[k].at[layer, h], v_ref.at[at], state_sem.at[slot, 3 * k + 2]))
        return copies

    def state_stores(g, kind):
        layer, h, slot = g // cuts, lax.rem(g, cuts), lax.rem(g, STAGED)
        copies = []
        for k in (2,) if kind else (0, 1):
            m_ref, v_ref = (m_b, v_b) if kind else (m_a, v_a)
            at = (slot,) if kind else (slot, k)
            copies.append(pltpu.make_async_copy(m_ref.at[at], new_m[k].at[layer, h], keep_sem.at[slot, 2 * k]))
            copies.append(pltpu.make_async_copy(v_ref.at[at], new_v[k].at[layer, h], keep_sem.at[slot, 2 * k + 1]))
        return copies

    def z_step(g, kind, s):
        slot = lax.rem(g, acc_slots)
        for way in (0, 1):
            t = Z - 1 - s + z if way == 0 else s - far

            def add(arrived, way=way, t=t):
                for i in (0, 1):
                    if kind:
                        total = f32(acc_b[slot, i, t]) + f32(all_b[g, i, t])
                        if arrived:
                            total += f32(z_b[g, way, s - 1, i])
                        acc_b[slot, i, t] = total.astype(jnp.bfloat16)
                    else:
                        total = f32(acc_a[slot, i, y, t]) + f32(all_a[g, i, y, t]) + f32(y_a[g, i, t])
                        if arrived:
                            total += f32(z_a[g, way, s - 1, i])
                        acc_a[slot, i, y, t] = total.astype(jnp.bfloat16)
                z_copy(g, kind, way, s).start()

            pl.when(place[way] == 0)(functools.partial(add, False))
            if s:
                pl.when((place[way] >= 1) & (place[way] <= s))(functools.partial(add, True))

    def z_wait(g, kind, s):
        for way in (0, 1):

            @pl.when((place[way] >= 1) & (place[way] <= s + 1))
            def _(way=way):
                ref = z_b.at[g, way, s] if kind else z_a.at[g, way, s]
                send_to(beside[way], ref, ref, z_send.at[0, kind, way, s], z_recv.at[g, kind, way, s]).wait_recv()

            @pl.when(place[way] <= s)
            def _(way=way):
                @pl.when(place[way] < Z - 1)
                def _():
                    z_copy(g, kind, way, s).wait_send()

    def spread_step(g, kind, s):
        for way in (0, 1):

            @pl.when((place[way] >= s) & (place[way] < Z - 1))
            def _(way=way):
                spread_copy(g, kind, way, s).start()

    def spread_wait(g, kind, s):
        for way in (0, 1):

            @pl.when(place[way] >= s + 1)
            def _(way=way):
                t = z - 1 - s if way == 0 else z + 1 + s
                ref = all_b.at[g, :, t] if kind else all_a.at[g, :, y, t]
                send_to(
                    beside[way], ref, ref, spread_send.at[lax.rem(g, 2), kind, way, s], spread_recv.at[g, kind, way, s]
                ).wait_recv()

            @pl.when((place[way] >= s) & (place[way] < Z - 1))
            def _(way=way):
                spread_copy(g, kind, way, s).wait_send()

    def arrived_along_z(up, down):
        up, down = f32(up), f32(down)
        return jnp.where(z >= 1, up, jnp.zeros_like(up)) + jnp.where(far >= 1, down, jnp.zeros_like(down))

    def adamw(total, w_ref, m_ref, v_ref, at):
        g = f32(total.astype(jnp.bfloat16))
        m = 0.9 * m_ref[at] + 0.1 * g
        v = 0.95 * v_ref[at] + 0.05 * g * g
        m_ref[at] = m
        v_ref[at] = v
        step = m * lax.rsqrt(v + 1e-8) + 0.1 * f32(w_ref[at])
        return f32(w_ref[at]) - 0.02 * step

    def stage_a(g, k):
        slot, staged = lax.rem(g, acc_slots), lax.rem(g, STAGED)
        if k == 1:
            for i in (0, 1):
                own_load(g, i).wait()
                pair_copy(g, i).wait_recv()
            for i in (0, 1):
                for t in range(Z):
                    acc_a[slot, i, 1 - y, t] = (f32(acc_a[slot, i, 1 - y, t]) + f32(all_a[g, i, 1 - y, t])).astype(jnp.bfloat16)
            y_copy(g, 0).start()
        if k == 2:
            for i in (0, 1):
                pair_copy(g, i).wait_send()
            y_copy(g, 0).wait()
            z_step(g, 0, 0)
        if k in (3, 4):
            z_wait(g, 0, k - 3)
            z_step(g, 0, k - 2)
        if k == 5:
            z_wait(g, 0, 2)
            for i in (0, 1):
                total = f32(acc_a[slot, i, y, z]) + f32(all_a[g, i, y, z]) + f32(y_a[g, i, z])
                total += arrived_along_z(z_a[g, 0, 2, i], z_a[g, 1, 2, i])
                all_a[g, i, y, z] = adamw(total, w_a, m_a, v_a, (staged, i)).astype(jnp.bfloat16)
            spread_step(g, 0, 0)
            for copy in state_stores(g, 0):
                copy.start()
        if k in (6, 7):
            spread_wait(g, 0, k - 6)
            spread_step(g, 0, k - 5)
        if k == 6:
            for copy in state_stores(g, 0):
                copy.wait()
        if k == 8:
            spread_wait(g, 0, 2)
            back_copy(g, 0).start()
            for i in (0, 1):
                out_copy(g, i, 0).start()
                out_store(g, i, 0).start()
        if k == 9:
            back_copy_recv = send_to(
                across, all_a.at[g, :, 1 - y], all_a.at[g, :, 1 - y], back_send.at[lax.rem(g, 2), 0], back_recv.at[g, 0]
            )
            back_copy_recv.wait_recv()
            back_copy(g, 0).wait_send()
            for i in (0, 1):
                out_copy(g, i, 1).start()
                out_store(g, i, 1).start()
        if k == 10:
            for i in (0, 1):
                for half in (0, 1):
                    out_copy(g, i, half).wait()
                    out_store(g, i, half).wait()

    def stage_b(g, k):
        slot, staged = lax.rem(g, acc_slots), lax.rem(g, STAGED)
        if k == 1:
            own_load(g, 2).wait()
            pair_copy(g, 2).wait_recv()
            z_step(g, 1, 0)
        if k == 2:
            pair_copy(g, 2).wait_send()
        if k in (2, 3):
            z_wait(g, 1, k - 2)
            z_step(g, 1, k - 1)
        if k == 4:
            z_wait(g, 1, 2)
            total = f32(acc_b[slot, 1 - y, z]) + f32(all_b[g, 1 - y, z])
            total += arrived_along_z(z_b[g, 0, 2, 1 - y], z_b[g, 1, 2, 1 - y])
            acc_b[slot, 1 - y, z] = total.astype(jnp.bfloat16)
            y_copy(g, 1).start()
        if k == 5:
            y_copy(g, 1).wait()
            total = f32(acc_b[slot, y, z]) + f32(all_b[g, y, z]) + f32(y_b[g])
            total += arrived_along_z(z_b[g, 0, 2, y], z_b[g, 1, 2, y])
            all_b[g, y, z] = adamw(total, w_b, m_b, v_b, (staged,)).astype(jnp.bfloat16)
            back_copy(g, 1).start()
            for copy in state_stores(g, 1):
                copy.start()
        if k == 6:
            for copy in state_stores(g, 1):
                copy.wait()
            send_to(
                across, all_b.at[g, 1 - y, z], all_b.at[g, 1 - y, z], back_send.at[lax.rem(g, 2), 1], back_recv.at[g, 1]
            ).wait_recv()
            back_copy(g, 1).wait_send()
            spread_step(g, 1, 0)
        if k in (7, 8):
            spread_wait(g, 1, k - 7)
            spread_step(g, 1, k - 6)
        if k == 9:
            spread_wait(g, 1, 2)
            out_copy(g, 2, 0).start()
            out_store(g, 2, 0).start()
        if k == 10:
            out_copy(g, 2, 0).wait()
            out_store(g, 2, 0).wait()

    def enter(g):
        for k in range(3):
            pair_copy(g, k).start()
        for k in range(3):
            own_load(g, k).start()

    barrier = pltpu.get_barrier_semaphore()
    for device in (partner, across):
        pl.semaphore_signal(barrier, inc=1, device_id=(rep, device), device_id_type=MESH)
    for way in (0, 1):

        @pl.when(place[way] < Z - 1)
        def _(way=way):
            pl.semaphore_signal(barrier, inc=1, device_id=(rep, beside[way]), device_id_type=MESH)

    pl.semaphore_wait(barrier, 4 - jnp.where(z == 0, 1, 0) - jnp.where(far == 0, 1, 0))

    enter(0)
    enter(1)

    @pl.loop(0, groups + STAGES - 1)
    def _(tick):
        for k in range(STAGES, 0, -1):
            g = tick - (k - 1)

            @pl.when((g >= 0) & (g < groups))
            def _(g=g, k=k):
                if k == 5:
                    for copy in state_loads(g):
                        copy.wait()
                stage_a(g, k)
                stage_b(g, k)
                if k == 3:
                    for copy in state_loads(g):
                        copy.start()

        @pl.when(tick + 2 < groups)
        def _():
            enter(tick + 2)


def update(terms, weights, m, v, cuts=CUTS):
    layers = weights[0].shape[0]
    groups = layers * cuts
    acc_slots = min(ACC, groups)
    full, own = [], []
    for w in weights:
        rows = w.shape[1] // (2 * Y * Z * cuts)
        full.append((layers, Y, Z, 2, cuts, rows, w.shape[2]))
        own.append((layers, cuts, rows, w.shape[2]))
    a, b = full[0][-2:], full[2][-2:]
    bf16, dma = jnp.bfloat16, pltpu.SemaphoreType.DMA
    anywhere = pl.BlockSpec(memory_space=pl.ANY)
    out = pl.pallas_call(
        functools.partial(kernel, groups, cuts, acc_slots),
        out_shape=[jax.ShapeDtypeStruct(s, bf16) for s in full] + [jax.ShapeDtypeStruct(s, jnp.float32) for s in own] * 2,
        in_specs=[anywhere] * 12,
        out_specs=[anywhere] * 9,
        scratch_shapes=[
            pltpu.VMEM((acc_slots, 2, Y, Z, *a), bf16),
            pltpu.VMEM((acc_slots, Y, Z, *b), bf16),
            pltpu.VMEM((groups, 2, Y, Z, *a), bf16),
            pltpu.VMEM((groups, Y, Z, *b), bf16),
            pltpu.VMEM((groups, 2, Z, *a), bf16),
            pltpu.VMEM((groups, *b), bf16),
            pltpu.VMEM((groups, 2, Z - 1, 2, *a), bf16),
            pltpu.VMEM((groups, 2, Z - 1, Y, *b), bf16),
            pltpu.VMEM((STAGED, 2, *a), bf16),
            pltpu.VMEM((STAGED, *b), bf16),
            *[pltpu.VMEM((STAGED, *s), jnp.float32) for _ in range(2) for s in ((2, *a), b)],
            dma((4, 3)),
            dma((4, 3)),
            dma((groups, 3)),
            dma((2, 2)),
            dma((groups, 2)),
            dma((2, 2, 2, Z - 1)),
            dma((groups, 2, 2, Z - 1)),
            dma((2, 2, 2, Z - 1)),
            dma((groups, 2, 2, Z - 1)),
            dma((2, 2)),
            dma((groups, 2)),
            dma((2, 5)),
            dma((groups, 5)),
            dma((2, 5)),
            dma((STAGED, 9)),
            dma((STAGED, 6)),
        ],
        compiler_params=pltpu.CompilerParams(collective_id=0, has_side_effects=True, vmem_limit_bytes=66_000_000),
        name="sum_step_spread",
    )(
        *[t.reshape(s) for t, s in zip(terms, full, strict=True)],
        *[w.reshape(s) for w, s in zip(weights, full, strict=True)],
        *[x.reshape(s) for x, s in zip(m, own, strict=True)],
        *[x.reshape(s) for x, s in zip(v, own, strict=True)],
    )
    return (
        *[o.reshape(w.shape) for o, w in zip(out[:3], weights, strict=True)],
        *[o.reshape(x.shape) for o, x in zip(out[3:6], m, strict=True)],
        *[o.reshape(x.shape) for o, x in zip(out[6:], v, strict=True)],
    )


def solution(mesh):
    def step(*arrays):
        terms, weights, m, v = (arrays[i : i + 3] for i in (0, 3, 6, 9))
        return update([t[0] for t in terms], weights, m, v)

    all_of, cut = P(None, None, None), P(None, "dp", None)
    return jax.shard_map(
        step,
        mesh=mesh,
        in_specs=(P(("rep", "dp"), None, None, None),) * 3 + (all_of,) * 3 + (cut,) * 6,
        out_specs=(P("rep", None, None),) * 3 + (P("rep", "dp", None),) * 6,
        check_vma=False,
    )
```

```python
import functools

import jax
import jax.numpy as jnp
from jax import lax
from jax.experimental import pallas as pl
from jax.experimental.pallas import tpu as pltpu
from jax.sharding import PartitionSpec as P

MESH = pl.DeviceIdType.MESH
Y, Z = 2, 4
ROWS, COLS = 8, 2
ACC = 6
SLOTS = 10
Y_SLOTS, UP_SLOTS, DOWN_SLOTS = 9, 5, 7
STAGED = 4
STAGES = 10
PAIR, DOWN, GATE, UP = range(4)
APART = (0, 10, 16, 22)
VMEM_BYTES = 13 * 2**20
PUT_BYTES = 13 * 2**20
ORDER = (
    (0, 1), (1, 1), (1, 2), (0, 8), (1, 3), (1, 4), (0, 7), (0, 10), (0, 9), (1, 9), (1, 8), (0, 4), (1, 7), (1, 10), (1, 5), (0, 6), (0, 3), (1, 6), (0, 5), (0, 2),
)


def kernel(groups, rows, cols, apart, *refs):
    terms, weights, moments_m, moments_v = (refs[i : i + 3] for i in (0, 3, 6, 9))
    mine_a, mine_b, theirs_a, theirs_b = refs[12:16]
    new_m, new_v = refs[16:19], refs[19:22]
    acc_a, acc_b, y_a, y_b, y_c, z_a, z_b, z_c, w_a, w_b, m_a, m_b, v_a, v_b = refs[22:36]
    load_sem, pair_send, pair_recv, y_send, y_recv, z_send, z_recv, spread_send, spread_recv = refs[36:45]
    back_send, back_recv, out_send, out_recv, state_sem, keep_sem = refs[45:51]

    rep, me = lax.axis_index("rep"), lax.axis_index("dp")
    c = lax.rem(me, 2)
    z = lax.rem(me // 2, Z)
    y = me // (2 * Z)
    far = Z - 1 - z
    partner = me + 1 - 2 * c
    across = me + (1 - 2 * y) * (2 * Z)
    beside = (me + 2, me - 2)
    place = (z, far)

    def send_to(device, src, dst, send_sem, recv_sem):
        return pltpu.make_async_remote_copy(
            src_ref=src, dst_ref=dst, send_sem=send_sem, recv_sem=recv_sem, device_id=(rep, device), device_id_type=MESH
        )

    def f32(x):
        return x.astype(jnp.float32)

    def part(g, ref):
        width = ref.shape[-1] // cols
        h = lax.rem(g, rows * cols)
        return g // (rows * cols), h // cols, pl.ds(pl.multiple_of(lax.rem(h, cols) * width, width), width)

    def z_first(kind):
        return kind in (DOWN, UP)

    def which(kind):
        return pl.ds(0, 2) if kind == PAIR else pl.ds(0, 1) if kind == GATE else 1

    def new_at(g, kind, *at, theirs=False):
        ref = (theirs_b if theirs else mine_b) if kind == DOWN else theirs_a if theirs else mine_a
        layer, h, width = part(g, ref)
        return ref.at[layer, *at, h, :, width] if kind == DOWN else ref.at[which(kind), layer, *at, h, :, width]

    def new_index(g, weight, i, t):
        layer, h, width = part(g, mine_b if weight == 2 else mine_a)
        return (layer, i, t, h, slice(None), width) if weight == 2 else (weight, layer, i, t, h, slice(None), width)

    def acc_at(g, kind, *at):
        slot = lax.rem(g, ACC)
        return acc_b.at[slot, *at] if kind == DOWN else acc_a.at[slot, which(kind), *at]

    def summed(g, weight, i, t):
        slot, here = lax.rem(g, ACC), new_index(g, weight, i, t)
        if weight == 2:
            return f32(acc_b[slot, i, t]) + f32(mine_b[here])
        return f32(acc_a[slot, weight, i, t]) + f32(mine_a[here])

    def keep(g, weight, i, t, total):
        slot = lax.rem(g, ACC)
        if weight == 2:
            acc_b[slot, i, t] = total.astype(jnp.bfloat16)
        else:
            acc_a[slot, weight, i, t] = total.astype(jnp.bfloat16)

    def own_load(g, k):
        layer, h, width = part(g, terms[k])
        dst = acc_b.at[lax.rem(g, ACC)] if k == 2 else acc_a.at[lax.rem(g, ACC), k]
        return pltpu.make_async_copy(terms[k].at[layer, :, :, c, h, :, width], dst, load_sem.at[lax.rem(g, 4), k])

    def pair_copy(g, k):
        layer, h, width = part(g, terms[k])
        src = terms[k].at[layer, :, :, 1 - c, h, :, width]
        dst = mine_b.at[layer, :, :, h, :, width] if k == 2 else mine_a.at[k, layer, :, :, h, :, width]
        return send_to(partner, src, dst, pair_send.at[lax.rem(g, 4), k], pair_recv.at[lax.rem(g, SLOTS), k])

    def slot_of(g, kind):
        if kind == DOWN:
            return lax.rem(g, DOWN_SLOTS)
        return lax.rem(sum(jnp.where(g > one, 1, 0) for one in apart), 2) if kind == UP else lax.rem(g, UP_SLOTS)

    def y_copy(g, kind):
        slot = lax.rem(g, SLOTS)
        if z_first(kind):
            src, dst = acc_at(g, kind, 1 - y, z), (y_b if kind == DOWN else y_c).at[slot_of(g, kind)]
        else:
            src, dst = acc_at(g, kind, 1 - y), y_a.at[lax.rem(g, Y_SLOTS), which(kind)]
        i = kind % 2 + kind // 3
        return send_to(across, src, dst, y_send.at[lax.rem(g, 2), i], y_recv.at[slot, i])

    def z_slot(g, kind, way, s):
        slot = slot_of(g, kind)
        if kind == DOWN:
            return z_b.at[slot, way, s]
        return z_c.at[slot, way, s] if kind == UP else z_a.at[slot, way, s, which(kind)]

    def z_copy(g, kind, way, s):
        t = Z - 1 - s + z if way == 0 else s - far
        src = acc_at(g, kind, slice(None), t) if z_first(kind) else acc_at(g, kind, y, t)
        i = kind % 2 + kind // 3
        sems = z_send.at[lax.rem(g, 2), i, way, s], z_recv.at[lax.rem(g, SLOTS), i, way, s]
        return send_to(beside[way], src, z_slot(g, kind, way, s), *sems)

    def spread_copy(g, kind, way, s, t):
        ref = new_at(g, kind, slice(None) if z_first(kind) else y, t)
        i = kind % 2 + kind // 3
        sems = spread_send.at[lax.rem(g, 2), i, way, s], spread_recv.at[lax.rem(g, SLOTS), i, way, s]
        return send_to(beside[way], ref, ref, *sems)

    def back_copy(g, kind, i, t):
        ref = new_at(g, kind, i, t)
        at = Z + kind // 3 if z_first(kind) else t
        return send_to(across, ref, ref, back_send.at[lax.rem(g, 2), at], back_recv.at[lax.rem(g, SLOTS), at])

    def out_copy(g, kind, half):
        at = slice(None) if z_first(kind) else 1 - y if half else y
        i = 2 + kind // 3 if z_first(kind) else half
        src, dst = new_at(g, kind, at, slice(None)), new_at(g, kind, at, slice(None), theirs=True)
        return send_to(partner, src, dst, out_send.at[lax.rem(g, 2), i], out_recv.at[lax.rem(g, SLOTS), i])

    def staged(g, k):
        slot = lax.rem(g, STAGED)
        return (w_b.at[slot], m_b.at[slot], v_b.at[slot]) if k == 2 else (w_a.at[slot, k], m_a.at[slot, k], v_a.at[slot, k])

    def state_loads(g, some):
        slot, copies = lax.rem(g, STAGED), []
        for k in some:
            layer, h, width = part(g, weights[k])
            w_ref, m_ref, v_ref = staged(g, k)
            copies.append(pltpu.make_async_copy(weights[k].at[layer, y, z, c, h, :, width], w_ref, state_sem.at[slot, 3 * k]))
            copies.append(pltpu.make_async_copy(moments_m[k].at[layer, h, :, width], m_ref, state_sem.at[slot, 3 * k + 1]))
            copies.append(pltpu.make_async_copy(moments_v[k].at[layer, h, :, width], v_ref, state_sem.at[slot, 3 * k + 2]))
        return copies

    def state_stores(g, k):
        layer, h, width = part(g, moments_m[k])
        _, m_ref, v_ref = staged(g, k)
        sems = keep_sem.at[lax.rem(g, STAGED), 2 * k], keep_sem.at[lax.rem(g, STAGED), 2 * k + 1]
        return (
            pltpu.make_async_copy(m_ref, new_m[k].at[layer, h, :, width], sems[0]),
            pltpu.make_async_copy(v_ref, new_v[k].at[layer, h, :, width], sems[1]),
        )

    def z_step(g, kind, s):
        slot = slot_of(g, kind)
        for way in (0, 1):
            t = Z - 1 - s + z if way == 0 else s - far

            def add(arrived, way=way, t=t):
                if z_first(kind):
                    weight = 2 if kind == DOWN else 1
                    came = z_b if kind == DOWN else z_c
                    for i in range(Y):
                        total = summed(g, weight, i, t)
                        if arrived:
                            total += f32(came[slot, way, s - 1, i])
                        keep(g, weight, i, t, total)
                else:
                    for weight in (0, 1) if kind == PAIR else (0,):
                        total = summed(g, weight, y, t) + f32(y_a[lax.rem(g, Y_SLOTS), weight, t])
                        if arrived:
                            total += f32(z_a[slot, way, s - 1, weight])
                        keep(g, weight, y, t, total)
                z_copy(g, kind, way, s).start()

            pl.when(place[way] == 0)(functools.partial(add, False))
            if s:
                pl.when((place[way] >= 1) & (place[way] <= s))(functools.partial(add, True))

    def z_wait(g, kind, s):
        i = kind % 2 + kind // 3
        for way in (0, 1):

            @pl.when((place[way] >= 1) & (place[way] <= s + 1))
            def _(way=way):
                ref = z_slot(g, kind, way, s)
                send_to(beside[way], ref, ref, z_send.at[0, i, way, s], z_recv.at[lax.rem(g, SLOTS), i, way, s]).wait_recv()

            @pl.when((place[way] <= s) & (place[way] < Z - 1))
            def _(way=way):
                z_copy(g, kind, way, s).wait_send()

    def spread_step(g, kind, s):
        for way in (0, 1):

            @pl.when((place[way] >= s) & (place[way] < Z - 1))
            def _(way=way):
                spread_copy(g, kind, way, s, z - s if way == 0 else z + s).start()

    def spread_wait(g, kind, s):
        for way in (0, 1):

            @pl.when(place[way] >= s + 1)
            def _(way=way):
                t = z - 1 - s if way == 0 else z + 1 + s
                spread_copy(g, kind, way, s, t).wait_recv()
                if not z_first(kind):
                    back_copy(g, kind, y, t).start()

            @pl.when((place[way] >= s) & (place[way] < Z - 1))
            def _(way=way):
                spread_copy(g, kind, way, s, z - s if way == 0 else z + s).wait_send()

    def along_z(came, g, kind, *at):
        slot = slot_of(g, kind)
        up, down = f32(came[slot, 0, Z - 2, *at]), f32(came[slot, 1, Z - 2, *at])
        return jnp.where(z >= 1, up, jnp.zeros_like(up)) + jnp.where(far >= 1, down, jnp.zeros_like(down))

    def adamw(g, weight, total):
        w_ref, m_ref, v_ref = staged(g, weight)
        w = f32(w_ref[...])
        gradient = f32(total.astype(jnp.bfloat16))
        m = 0.9 * m_ref[...] + 0.1 * gradient
        v = 0.95 * v_ref[...] + 0.05 * gradient * gradient
        m_ref[...] = m
        v_ref[...] = v
        new = (w - 0.02 * (m * lax.rsqrt(v + 1e-8) + 0.1 * w)).astype(jnp.bfloat16)
        if weight == 2:
            mine_b[new_index(g, weight, y, z)] = new
        else:
            mine_a[new_index(g, weight, y, z)] = new

    def y_first_stage(g, kind, k):
        some = (0, 1) if kind == PAIR else (0,)
        if k == 1:
            for i in some:
                own_load(g, i).wait()
                pair_copy(g, i).wait_recv()
            for i in some:
                for t in range(Z):
                    keep(g, i, 1 - y, t, summed(g, i, 1 - y, t))
            y_copy(g, kind).start()
        if k == 2:
            for i in some:
                pair_copy(g, i).wait_send()
            y_copy(g, kind).wait()
            z_step(g, kind, 0)
        if k in (3, 4):
            z_wait(g, kind, k - 3)
            z_step(g, kind, k - 2)
        if k == 5:
            z_wait(g, kind, 2)
            for i in some:
                adamw(g, i, summed(g, i, y, z) + f32(y_a[lax.rem(g, Y_SLOTS), i, z]) + along_z(z_a, g, kind, i))
            spread_step(g, kind, 0)
            back_copy(g, kind, y, z).start()
            for i in some:
                for copy in state_stores(g, i):
                    copy.start()
        if k in (6, 7):
            spread_wait(g, kind, k - 6)
            spread_step(g, kind, k - 5)
        if k == 6:
            for i in some:
                for copy in state_stores(g, i):
                    copy.wait()
        if k == 8:
            spread_wait(g, kind, 2)
            out_copy(g, kind, 0).start()
        if k == 9:
            for t in range(Z):
                back_copy(g, kind, 1 - y, t).wait_recv()
                back_copy(g, kind, y, t).wait_send()
            out_copy(g, kind, 1).start()
        if k == 10:
            for half in (0, 1):
                out_copy(g, kind, half).wait()

    def z_first_stage(g, kind, k):
        weight = 2 if kind == DOWN else 1
        came = z_b if kind == DOWN else z_c
        if k == 1:
            own_load(g, weight).wait()
            pair_copy(g, weight).wait_recv()
            z_step(g, kind, 0)
        if k == 2:
            pair_copy(g, weight).wait_send()
        if k in (2, 3):
            z_wait(g, kind, k - 2)
            z_step(g, kind, k - 1)
        if k == 4:
            z_wait(g, kind, 2)
            keep(g, weight, 1 - y, z, summed(g, weight, 1 - y, z) + along_z(came, g, kind, 1 - y))
            y_copy(g, kind).start()
        if k == 5:
            y_copy(g, kind).wait()
            arrived = f32((y_b if kind == DOWN else y_c)[slot_of(g, kind)])
            adamw(g, weight, summed(g, weight, y, z) + arrived + along_z(came, g, kind, y))
            back_copy(g, kind, y, z).start()
            for copy in state_stores(g, weight):
                copy.start()
        if k == 6:
            back_copy(g, kind, 1 - y, z).wait_recv()
            back_copy(g, kind, y, z).wait_send()
            spread_step(g, kind, 0)
            for copy in state_stores(g, weight):
                copy.wait()
        if k in (7, 8):
            spread_wait(g, kind, k - 7)
            spread_step(g, kind, k - 6)
        if k == 9:
            spread_wait(g, kind, 2)
            out_copy(g, kind, 0).start()
        if k == 10:
            out_copy(g, kind, 0).wait()

    def is_apart(g):
        found = g < 0
        for one in apart:
            found = found | (g == one)
        return found

    def enter(g):
        for k in range(3):
            pair_copy(g, k).start()
        for k in range(3):
            own_load(g, k).start()

    barrier = pltpu.get_barrier_semaphore()
    for device in (partner, across):
        pl.semaphore_signal(barrier, inc=1, device_id=(rep, device), device_id_type=MESH)
    for way in (0, 1):

        @pl.when(place[way] < Z - 1)
        def _(way=way):
            pl.semaphore_signal(barrier, inc=1, device_id=(rep, beside[way]), device_id_type=MESH)

    pl.semaphore_wait(barrier, 4 - jnp.where(z == 0, 1, 0) - jnp.where(far == 0, 1, 0))

    enter(0)
    enter(1)

    @pl.loop(0, groups + STAGES - 1)
    def _(tick):
        for kind, k in ORDER:
            g = tick - (k - 1)

            @pl.when((g >= 0) & (g < groups))
            def _(g=g, k=k, kind=kind):
                if k == 3 or k == 5:
                    for copy in state_loads(g, (2,) if kind else (0, 1)):
                        if k == 3:
                            copy.start()
                        else:
                            copy.wait()
                if kind == 1:
                    z_first_stage(g, DOWN, k)
                elif apart:
                    here = is_apart(g)

                    @pl.when(jnp.logical_not(here))
                    def _():
                        y_first_stage(g, PAIR, k)

                    @pl.when(here)
                    def _():
                        y_first_stage(g, GATE, k)
                        z_first_stage(g, UP, k)

                else:
                    y_first_stage(g, PAIR, k)

        @pl.when(tick + 2 < groups)
        def _():
            enter(tick + 2)


def put(*refs):
    halves, moments = (refs[0:2], refs[2:4]), refs[4:10]
    outs, rooms, sem = refs[10:19], refs[19:25], refs[25]
    c = lax.rem(lax.axis_index("dp"), 2)
    pairs = []
    for core, (a, b) in zip((c, 1 - c), halves, strict=True):
        for layer in range(b.shape[0]):
            sources = a.at[0, layer], a.at[1, layer], b.at[layer]
            pairs += [(src, out.at[layer, :, :, core]) for src, out in zip(sources, outs[:3], strict=True)]
    came = [pltpu.make_async_copy(src, room, sem.at[n]) for n, (src, room) in enumerate(zip(moments, rooms, strict=True))]
    gone = [pltpu.make_async_copy(room, out, sem.at[6 + n]) for n, (room, out) in enumerate(zip(rooms, outs[3:], strict=True))]
    copies = [pltpu.make_async_copy(src, dst, sem.at[12 + n]) for n, (src, dst) in enumerate(pairs)]
    for copy in came + copies:
        copy.start()
    for first, then in zip(came, gone, strict=True):
        first.wait()
        then.start()
    for copy in copies + gone:
        copy.wait()


def in_hbm(x):
    return pltpu.with_memory_space_constraint(x, pltpu.HBM)


def update(terms, weights, m, v, rows=ROWS, cols=COLS, apart=APART):
    layers = weights[0].shape[0]
    groups = layers * rows * cols
    full, own = [], []
    for w in weights:
        lines = w.shape[1] // (2 * Y * Z * rows)
        full.append((layers, Y, Z, 2, rows, lines, w.shape[2]))
        own.append((layers, rows, lines, w.shape[2]))
    halves = (2, *full[0][:3], *full[0][4:]), (*full[2][:3], *full[2][4:])
    a, b = ((s[-2], s[-1] // cols) for s in (full[0], full[2]))
    bf16, dma = jnp.bfloat16, pltpu.SemaphoreType.DMA
    anywhere, vmem = pl.BlockSpec(memory_space=pl.ANY), pl.BlockSpec(memory_space=pltpu.VMEM)
    held = pl.pallas_call(
        functools.partial(kernel, groups, rows, cols, apart),
        out_shape=[pltpu.VMEM(s, bf16) for s in halves] * 2
        + [pltpu.HBM(s, jnp.float32) for s in own] * 2,
        in_specs=[anywhere] * 12,
        out_specs=[vmem] * 4 + [pl.BlockSpec(memory_space=pltpu.HBM)] * 6,
        scratch_shapes=[
            pltpu.VMEM((ACC, 2, Y, Z, *a), bf16),
            pltpu.VMEM((ACC, Y, Z, *b), bf16),
            pltpu.VMEM((Y_SLOTS, 2, Z, *a), bf16),
            pltpu.VMEM((DOWN_SLOTS, *b), bf16),
            pltpu.VMEM((2, *a), bf16),
            pltpu.VMEM((UP_SLOTS, 2, Z - 1, 2, *a), bf16),
            pltpu.VMEM((DOWN_SLOTS, 2, Z - 1, Y, *b), bf16),
            pltpu.VMEM((2, 2, Z - 1, Y, *a), bf16),
            pltpu.VMEM((STAGED, 2, *a), bf16),
            pltpu.VMEM((STAGED, *b), bf16),
            *[pltpu.VMEM((STAGED, *s), jnp.float32) for _ in range(2) for s in ((2, *a), b)],
            dma((4, 3)),
            dma((4, 3)),
            dma((SLOTS, 3)),
            dma((2, 3)),
            dma((SLOTS, 3)),
            dma((2, 3, 2, Z - 1)),
            dma((SLOTS, 3, 2, Z - 1)),
            dma((2, 3, 2, Z - 1)),
            dma((SLOTS, 3, 2, Z - 1)),
            dma((2, Z + 2)),
            dma((SLOTS, Z + 2)),
            dma((2, 4)),
            dma((SLOTS, 4)),
            dma((STAGED, 9)),
            dma((STAGED, 6)),
        ],
        compiler_params=pltpu.CompilerParams(collective_id=0, has_side_effects=True, vmem_limit_bytes=VMEM_BYTES),
        name="sum_step_spread",
    )(
        *[in_hbm(t.reshape(s)) for t, s in zip(terms, full, strict=True)],
        *[in_hbm(w.reshape(s)) for w, s in zip(weights, full, strict=True)],
        *[in_hbm(x.reshape(s)) for x, s in zip(m, own, strict=True)],
        *[in_hbm(x.reshape(s)) for x, s in zip(v, own, strict=True)],
    )
    out = pl.pallas_call(
        put,
        out_shape=[jax.ShapeDtypeStruct(s, bf16) for s in full] + [jax.ShapeDtypeStruct(s, jnp.float32) for s in own] * 2,
        in_specs=[vmem] * 4 + [anywhere] * 6,
        out_specs=[anywhere] * 9,
        scratch_shapes=[*[pltpu.VMEM(s, jnp.float32) for s in own] * 2, dma((12 + 6 * layers,))],
        compiler_params=pltpu.CompilerParams(vmem_limit_bytes=PUT_BYTES),
        name="put",
    )(*held[:4], *[in_hbm(x) for x in held[4:]])
    return (
        *[o.reshape(w.shape) for o, w in zip(out[:3], weights, strict=True)],
        *[o.reshape(x.shape) for o, x in zip(out[3:6], m, strict=True)],
        *[o.reshape(x.shape) for o, x in zip(out[6:], v, strict=True)],
    )


def solution(mesh):
    def step(*arrays):
        terms, weights, m, v = (arrays[i : i + 3] for i in (0, 3, 6, 9))
        return update([t[0] for t in terms], weights, m, v)

    all_of, cut = P(None, None, None), P(None, "dp", None)
    return jax.shard_map(
        step,
        mesh=mesh,
        in_specs=(P(("rep", "dp"), None, None, None),) * 3 + (all_of,) * 3 + (cut,) * 6,
        out_specs=(P("rep", None, None),) * 3 + (P("rep", "dp", None),) * 6,
        check_vma=False,
    )
```

```python
import functools

import jax
import jax.numpy as jnp
from jax import lax
from jax.experimental import pallas as pl
from jax.experimental.pallas import tpu as pltpu
from jax.sharding import PartitionSpec as P

MESH = pl.DeviceIdType.MESH
Y, Z = 2, 4
ROWS, COLS = 8, 2
SLOTS = 10
Y_SLOTS, UP_SLOTS, DOWN_SLOTS = 9, 5, 7
STAGED = 4
STAGES = 10
PAIR, DOWN, GATE, UP = range(4)
APART = (0, 10, 16, 22)
VMEM_BYTES = 8 * 2**20
ORDER = (
    (0, 1), (1, 1), (1, 2), (0, 8), (1, 3), (1, 4), (0, 7), (0, 10), (0, 9), (1, 9), (1, 8), (0, 4), (1, 7), (1, 10), (1, 5), (0, 6), (0, 3), (1, 6), (0, 5), (0, 2),
)


def kernel(groups, rows, cols, apart, *refs):
    terms, weights, moments_m, moments_v = (refs[i : i + 3] for i in (0, 3, 6, 9))
    mine_a, mine_b, theirs_a, theirs_b = refs[12:16]
    m_a, m_b, v_a, v_b = refs[16:20]
    y_a, y_b, y_c, z_a, z_b, z_c, w_a, w_b = refs[20:28]
    load_sem, pair_send, pair_recv, y_send, y_recv, z_send, z_recv, spread_send, spread_recv = refs[28:37]
    back_send, back_recv, out_send, out_recv, state_sem, free_sem = refs[37:43]

    rep, me = lax.axis_index("rep"), lax.axis_index("dp")
    c = lax.rem(me, 2)
    z = lax.rem(me // 2, Z)
    y = me // (2 * Z)
    far = Z - 1 - z
    partner = me + 1 - 2 * c
    across = me + (1 - 2 * y) * (2 * Z)
    beside = (me + 2, me - 2)
    place = (z, far)

    def send_to(device, src, dst, send_sem, recv_sem):
        return pltpu.make_async_remote_copy(
            src_ref=src, dst_ref=dst, send_sem=send_sem, recv_sem=recv_sem, device_id=(rep, device), device_id_type=MESH
        )

    def f32(x):
        return x.astype(jnp.float32)

    def part(g, ref):
        width = ref.shape[-1] // cols
        h = lax.rem(g, rows * cols)
        return g // (rows * cols), h // cols, pl.ds(pl.multiple_of(lax.rem(h, cols) * width, width), width)

    def z_first(kind):
        return kind in (DOWN, UP)

    def which(kind):
        return pl.ds(0, 2) if kind == PAIR else pl.ds(0, 1) if kind == GATE else 1

    def new_at(g, kind, *at, theirs=False):
        ref = (theirs_b if theirs else mine_b) if kind == DOWN else theirs_a if theirs else mine_a
        layer, h, width = part(g, ref)
        return ref.at[layer, *at, h, :, width] if kind == DOWN else ref.at[which(kind), layer, *at, h, :, width]

    def new_index(g, weight, i, t):
        layer, h, width = part(g, mine_b if weight == 2 else mine_a)
        return (layer, i, t, h, slice(None), width) if weight == 2 else (weight, layer, i, t, h, slice(None), width)

    def acc_at(g, kind, *at):
        return new_at(g, kind, *at, theirs=True)

    def summed(g, weight, i, t):
        here = new_index(g, weight, i, t)
        return f32(theirs_b[here]) + f32(mine_b[here]) if weight == 2 else f32(theirs_a[here]) + f32(mine_a[here])

    def keep(g, weight, i, t, total):
        if weight == 2:
            theirs_b[new_index(g, weight, i, t)] = total.astype(jnp.bfloat16)
        else:
            theirs_a[new_index(g, weight, i, t)] = total.astype(jnp.bfloat16)

    def tell_partner(kind):
        pl.semaphore_signal(free_sem.at[kind % 2 + kind // 3], inc=1, device_id=(rep, partner), device_id_type=MESH)

    def hear_partner(kind):
        pl.semaphore_wait(free_sem.at[kind % 2 + kind // 3], 1)

    def own_load(g, k):
        layer, h, width = part(g, terms[k])
        dst = theirs_b.at[layer, :, :, h, :, width] if k == 2 else theirs_a.at[k, layer, :, :, h, :, width]
        return pltpu.make_async_copy(terms[k].at[layer, :, :, c, h, :, width], dst, load_sem.at[lax.rem(g, 4), k])

    def pair_copy(g, k):
        layer, h, width = part(g, terms[k])
        src = terms[k].at[layer, :, :, 1 - c, h, :, width]
        dst = mine_b.at[layer, :, :, h, :, width] if k == 2 else mine_a.at[k, layer, :, :, h, :, width]
        return send_to(partner, src, dst, pair_send.at[lax.rem(g, 4), k], pair_recv.at[lax.rem(g, SLOTS), k])

    def slot_of(g, kind):
        if kind == DOWN:
            return lax.rem(g, DOWN_SLOTS)
        return lax.rem(sum(jnp.where(g > one, 1, 0) for one in apart), 2) if kind == UP else lax.rem(g, UP_SLOTS)

    def y_copy(g, kind):
        slot = lax.rem(g, SLOTS)
        if z_first(kind):
            src, dst = acc_at(g, kind, 1 - y, z), (y_b if kind == DOWN else y_c).at[slot_of(g, kind)]
        else:
            src, dst = acc_at(g, kind, 1 - y, slice(None)), y_a.at[lax.rem(g, Y_SLOTS), which(kind)]
        i = kind % 2 + kind // 3
        return send_to(across, src, dst, y_send.at[lax.rem(g, 2), i], y_recv.at[slot, i])

    def z_slot(g, kind, way, s):
        slot = slot_of(g, kind)
        if kind == DOWN:
            return z_b.at[slot, way, s]
        return z_c.at[slot, way, s] if kind == UP else z_a.at[slot, way, s, which(kind)]

    def z_copy(g, kind, way, s):
        t = Z - 1 - s + z if way == 0 else s - far
        src = acc_at(g, kind, slice(None), t) if z_first(kind) else acc_at(g, kind, y, t)
        i = kind % 2 + kind // 3
        sems = z_send.at[lax.rem(g, 2), i, way, s], z_recv.at[lax.rem(g, SLOTS), i, way, s]
        return send_to(beside[way], src, z_slot(g, kind, way, s), *sems)

    def spread_copy(g, kind, way, s, t):
        ref = new_at(g, kind, slice(None) if z_first(kind) else y, t)
        i = kind % 2 + kind // 3
        sems = spread_send.at[lax.rem(g, 2), i, way, s], spread_recv.at[lax.rem(g, SLOTS), i, way, s]
        return send_to(beside[way], ref, ref, *sems)

    def back_copy(g, kind, i, t):
        ref = new_at(g, kind, i, t)
        at = Z + kind // 3 if z_first(kind) else t
        return send_to(across, ref, ref, back_send.at[lax.rem(g, 2), at], back_recv.at[lax.rem(g, SLOTS), at])

    def out_copy(g, kind, half):
        at = slice(None) if z_first(kind) else 1 - y if half else y
        i = 2 + kind // 3 if z_first(kind) else half
        src, dst = new_at(g, kind, at, slice(None)), new_at(g, kind, at, slice(None), theirs=True)
        return send_to(partner, src, dst, out_send.at[lax.rem(g, 2), i], out_recv.at[lax.rem(g, SLOTS), i])

    def staged(g, k):
        slot = lax.rem(g, STAGED)
        layer, h, width = part(g, moments_m[k])
        at = (layer, h, slice(None), width) if k == 2 else (k, layer, h, slice(None), width)
        return (w_b.at[slot], m_b.at[at], v_b.at[at]) if k == 2 else (w_a.at[slot, k], m_a.at[at], v_a.at[at])

    def state_loads(g, some):
        slot, copies = lax.rem(g, STAGED), []
        for k in some:
            layer, h, width = part(g, weights[k])
            w_ref, m_ref, v_ref = staged(g, k)
            copies.append(pltpu.make_async_copy(weights[k].at[layer, y, z, c, h, :, width], w_ref, state_sem.at[slot, 3 * k]))
            copies.append(pltpu.make_async_copy(moments_m[k].at[layer, h, :, width], m_ref, state_sem.at[slot, 3 * k + 1]))
            copies.append(pltpu.make_async_copy(moments_v[k].at[layer, h, :, width], v_ref, state_sem.at[slot, 3 * k + 2]))
        return copies

    def z_step(g, kind, s):
        slot = slot_of(g, kind)
        for way in (0, 1):
            t = Z - 1 - s + z if way == 0 else s - far

            def add(arrived, way=way, t=t):
                if z_first(kind):
                    weight = 2 if kind == DOWN else 1
                    came = z_b if kind == DOWN else z_c
                    for i in range(Y):
                        total = summed(g, weight, i, t)
                        if arrived:
                            total += f32(came[slot, way, s - 1, i])
                        keep(g, weight, i, t, total)
                else:
                    for weight in (0, 1) if kind == PAIR else (0,):
                        total = summed(g, weight, y, t) + f32(y_a[lax.rem(g, Y_SLOTS), weight, t])
                        if arrived:
                            total += f32(z_a[slot, way, s - 1, weight])
                        keep(g, weight, y, t, total)
                z_copy(g, kind, way, s).start()

            pl.when(place[way] == 0)(functools.partial(add, False))
            if s:
                pl.when((place[way] >= 1) & (place[way] <= s))(functools.partial(add, True))

    def z_wait(g, kind, s):
        i = kind % 2 + kind // 3
        for way in (0, 1):

            @pl.when((place[way] >= 1) & (place[way] <= s + 1))
            def _(way=way):
                ref = z_slot(g, kind, way, s)
                send_to(beside[way], ref, ref, z_send.at[0, i, way, s], z_recv.at[lax.rem(g, SLOTS), i, way, s]).wait_recv()

            @pl.when((place[way] <= s) & (place[way] < Z - 1))
            def _(way=way):
                z_copy(g, kind, way, s).wait_send()

    def spread_step(g, kind, s):
        for way in (0, 1):

            @pl.when((place[way] >= s) & (place[way] < Z - 1))
            def _(way=way):
                spread_copy(g, kind, way, s, z - s if way == 0 else z + s).start()

    def spread_wait(g, kind, s):
        for way in (0, 1):

            @pl.when(place[way] >= s + 1)
            def _(way=way):
                t = z - 1 - s if way == 0 else z + 1 + s
                spread_copy(g, kind, way, s, t).wait_recv()
                if not z_first(kind):
                    back_copy(g, kind, y, t).start()

            @pl.when((place[way] >= s) & (place[way] < Z - 1))
            def _(way=way):
                spread_copy(g, kind, way, s, z - s if way == 0 else z + s).wait_send()

    def along_z(came, g, kind, *at):
        slot = slot_of(g, kind)
        up, down = f32(came[slot, 0, Z - 2, *at]), f32(came[slot, 1, Z - 2, *at])
        return jnp.where(z >= 1, up, jnp.zeros_like(up)) + jnp.where(far >= 1, down, jnp.zeros_like(down))

    def adamw(g, weight, total):
        w_ref, m_ref, v_ref = staged(g, weight)
        w = f32(w_ref[...])
        gradient = f32(total.astype(jnp.bfloat16))
        m = 0.9 * m_ref[...] + 0.1 * gradient
        v = 0.95 * v_ref[...] + 0.05 * gradient * gradient
        m_ref[...] = m
        v_ref[...] = v
        new = (w - 0.02 * (m * lax.rsqrt(v + 1e-8) + 0.1 * w)).astype(jnp.bfloat16)
        if weight == 2:
            mine_b[new_index(g, weight, y, z)] = new
        else:
            mine_a[new_index(g, weight, y, z)] = new

    def y_first_stage(g, kind, k):
        some = (0, 1) if kind == PAIR else (0,)
        if k == 1:
            for i in some:
                own_load(g, i).wait()
                pair_copy(g, i).wait_recv()
            for i in some:
                for t in range(Z):
                    keep(g, i, 1 - y, t, summed(g, i, 1 - y, t))
            y_copy(g, kind).start()
        if k == 2:
            for i in some:
                pair_copy(g, i).wait_send()
            y_copy(g, kind).wait()
            z_step(g, kind, 0)
        if k in (3, 4):
            z_wait(g, kind, k - 3)
            z_step(g, kind, k - 2)
        if k == 5:
            z_wait(g, kind, 2)
            for i in some:
                adamw(g, i, summed(g, i, y, z) + f32(y_a[lax.rem(g, Y_SLOTS), i, z]) + along_z(z_a, g, kind, i))
            spread_step(g, kind, 0)
            back_copy(g, kind, y, z).start()
            tell_partner(kind)
        if k in (6, 7):
            spread_wait(g, kind, k - 6)
            spread_step(g, kind, k - 5)
        if k == 8:
            spread_wait(g, kind, 2)
            hear_partner(kind)
            out_copy(g, kind, 0).start()
        if k == 9:
            for t in range(Z):
                back_copy(g, kind, 1 - y, t).wait_recv()
                back_copy(g, kind, y, t).wait_send()
            out_copy(g, kind, 1).start()
        if k == 10:
            for half in (0, 1):
                out_copy(g, kind, half).wait()

    def z_first_stage(g, kind, k):
        weight = 2 if kind == DOWN else 1
        came = z_b if kind == DOWN else z_c
        if k == 1:
            own_load(g, weight).wait()
            pair_copy(g, weight).wait_recv()
            z_step(g, kind, 0)
        if k == 2:
            pair_copy(g, weight).wait_send()
        if k in (2, 3):
            z_wait(g, kind, k - 2)
            z_step(g, kind, k - 1)
        if k == 4:
            z_wait(g, kind, 2)
            keep(g, weight, 1 - y, z, summed(g, weight, 1 - y, z) + along_z(came, g, kind, 1 - y))
            y_copy(g, kind).start()
        if k == 5:
            y_copy(g, kind).wait()
            arrived = f32((y_b if kind == DOWN else y_c)[slot_of(g, kind)])
            adamw(g, weight, summed(g, weight, y, z) + arrived + along_z(came, g, kind, y))
            back_copy(g, kind, y, z).start()
            tell_partner(kind)
        if k == 6:
            back_copy(g, kind, 1 - y, z).wait_recv()
            back_copy(g, kind, y, z).wait_send()
            spread_step(g, kind, 0)
        if k in (7, 8):
            spread_wait(g, kind, k - 7)
            spread_step(g, kind, k - 6)
        if k == 9:
            spread_wait(g, kind, 2)
            hear_partner(kind)
            out_copy(g, kind, 0).start()
        if k == 10:
            out_copy(g, kind, 0).wait()

    def is_apart(g):
        found = g < 0
        for one in apart:
            found = found | (g == one)
        return found

    def enter(g):
        for k in range(3):
            pair_copy(g, k).start()
        for k in range(3):
            own_load(g, k).start()

    barrier = pltpu.get_barrier_semaphore()
    for device in (partner, across):
        pl.semaphore_signal(barrier, inc=1, device_id=(rep, device), device_id_type=MESH)
    for way in (0, 1):

        @pl.when(place[way] < Z - 1)
        def _(way=way):
            pl.semaphore_signal(barrier, inc=1, device_id=(rep, beside[way]), device_id_type=MESH)

    pl.semaphore_wait(barrier, 4 - jnp.where(z == 0, 1, 0) - jnp.where(far == 0, 1, 0))

    enter(0)
    enter(1)

    @pl.loop(0, groups + STAGES - 1)
    def _(tick):
        for kind, k in ORDER:
            g = tick - (k - 1)

            @pl.when((g >= 0) & (g < groups))
            def _(g=g, k=k, kind=kind):
                if k == 3 or k == 5:
                    for copy in state_loads(g, (2,) if kind else (0, 1)):
                        if k == 3:
                            copy.start()
                        else:
                            copy.wait()
                if kind == 1:
                    z_first_stage(g, DOWN, k)
                elif apart:
                    here = is_apart(g)

                    @pl.when(jnp.logical_not(here))
                    def _():
                        y_first_stage(g, PAIR, k)

                    @pl.when(here)
                    def _():
                        y_first_stage(g, GATE, k)
                        z_first_stage(g, UP, k)

                else:
                    y_first_stage(g, PAIR, k)

        @pl.when(tick + 2 < groups)
        def _():
            enter(tick + 2)


def put(*refs):
    halves, moments = (refs[0:2], refs[2:4]), (refs[4:6], refs[6:8])
    outs, sem = refs[8:17], refs[17]
    c = lax.rem(lax.axis_index("dp"), 2)
    pairs = []
    for core, (a, b) in zip((c, 1 - c), halves, strict=True):
        for layer in range(b.shape[0]):
            sources = a.at[0, layer], a.at[1, layer], b.at[layer]
            pairs += [(src, out.at[layer, :, :, core]) for src, out in zip(sources, outs[:3], strict=True)]
    for i, (a, b) in enumerate(moments):
        pairs += zip((a.at[0], a.at[1], b), outs[3 + 3 * i : 6 + 3 * i], strict=True)
    copies = [pltpu.make_async_copy(src, dst, sem.at[n]) for n, (src, dst) in enumerate(pairs)]
    for copy in copies:
        copy.start()
    for copy in copies:
        copy.wait()


def in_hbm(x):
    return pltpu.with_memory_space_constraint(x, pltpu.HBM)


def update(terms, weights, m, v, rows=ROWS, cols=COLS, apart=APART):
    layers = weights[0].shape[0]
    groups = layers * rows * cols
    full, own = [], []
    for w in weights:
        lines = w.shape[1] // (2 * Y * Z * rows)
        full.append((layers, Y, Z, 2, rows, lines, w.shape[2]))
        own.append((layers, rows, lines, w.shape[2]))
    halves = (2, *full[0][:3], *full[0][4:]), (*full[2][:3], *full[2][4:])
    a, b = ((s[-2], s[-1] // cols) for s in (full[0], full[2]))
    bf16, dma = jnp.bfloat16, pltpu.SemaphoreType.DMA
    anywhere, vmem = pl.BlockSpec(memory_space=pl.ANY), pl.BlockSpec(memory_space=pltpu.VMEM)
    held = pl.pallas_call(
        functools.partial(kernel, groups, rows, cols, apart),
        out_shape=[pltpu.VMEM(s, bf16) for s in halves] * 2
        + [pltpu.VMEM(s, jnp.float32) for s in ((2, *own[0]), own[2])] * 2,
        in_specs=[anywhere] * 12,
        out_specs=[vmem] * 8,
        scratch_shapes=[
            pltpu.VMEM((Y_SLOTS, 2, Z, *a), bf16),
            pltpu.VMEM((DOWN_SLOTS, *b), bf16),
            pltpu.VMEM((2, *a), bf16),
            pltpu.VMEM((UP_SLOTS, 2, Z - 1, 2, *a), bf16),
            pltpu.VMEM((DOWN_SLOTS, 2, Z - 1, Y, *b), bf16),
            pltpu.VMEM((2, 2, Z - 1, Y, *a), bf16),
            pltpu.VMEM((STAGED, 2, *a), bf16),
            pltpu.VMEM((STAGED, *b), bf16),
            dma((4, 3)),
            dma((4, 3)),
            dma((SLOTS, 3)),
            dma((2, 3)),
            dma((SLOTS, 3)),
            dma((2, 3, 2, Z - 1)),
            dma((SLOTS, 3, 2, Z - 1)),
            dma((2, 3, 2, Z - 1)),
            dma((SLOTS, 3, 2, Z - 1)),
            dma((2, Z + 2)),
            dma((SLOTS, Z + 2)),
            dma((2, 4)),
            dma((SLOTS, 4)),
            dma((STAGED, 9)),
            pltpu.SemaphoreType.REGULAR((3,)),
        ],
        compiler_params=pltpu.CompilerParams(collective_id=0, has_side_effects=True, vmem_limit_bytes=VMEM_BYTES),
        name="sum_step_spread",
    )(
        *[in_hbm(t.reshape(s)) for t, s in zip(terms, full, strict=True)],
        *[in_hbm(w.reshape(s)) for w, s in zip(weights, full, strict=True)],
        *[in_hbm(x.reshape(s)) for x, s in zip(m, own, strict=True)],
        *[in_hbm(x.reshape(s)) for x, s in zip(v, own, strict=True)],
    )
    out = pl.pallas_call(
        put,
        out_shape=[jax.ShapeDtypeStruct(s, bf16) for s in full] + [jax.ShapeDtypeStruct(s, jnp.float32) for s in own] * 2,
        in_specs=[vmem] * 8,
        out_specs=[anywhere] * 9,
        scratch_shapes=[dma((6 + 6 * layers,))],
        compiler_params=pltpu.CompilerParams(vmem_limit_bytes=VMEM_BYTES),
        name="put",
    )(*held)
    return (
        *[o.reshape(w.shape) for o, w in zip(out[:3], weights, strict=True)],
        *[o.reshape(x.shape) for o, x in zip(out[3:6], m, strict=True)],
        *[o.reshape(x.shape) for o, x in zip(out[6:], v, strict=True)],
    )


def solution(mesh):
    def step(*arrays):
        terms, weights, m, v = (arrays[i : i + 3] for i in (0, 3, 6, 9))
        return update([t[0] for t in terms], weights, m, v)

    all_of, cut = P(None, None, None), P(None, "dp", None)
    return jax.shard_map(
        step,
        mesh=mesh,
        in_specs=(P(("rep", "dp"), None, None, None),) * 3 + (all_of,) * 3 + (cut,) * 6,
        out_specs=(P("rep", None, None),) * 3 + (P("rep", "dp", None),) * 6,
        check_vma=False,
    )
```

```python
import functools

import jax
import jax.numpy as jnp
from jax import lax
from jax.experimental import pallas as pl
from jax.experimental.pallas import tpu as pltpu
from jax.sharding import PartitionSpec as P

MESH = pl.DeviceIdType.MESH
Y, Z = 2, 4
ROWS, COLS = 8, 2
SLOTS = 10
Y_SLOTS, UP_SLOTS, DOWN_SLOTS = 9, 5, 7
STAGED = 4
STAGES = 10
BY_BLOCK = 3
PAIR, DOWN, GATE, UP = range(4)
APART = (0, 7, 11, 17, 21)
VMEM_BYTES = 8 * 2**20
ORDER = (
    (1, 7), (1, 5), (1, 6), (1, 4), (0, 8), (0, 7), (1, 3), (1, 9), (1, 8), (0, 1), (0, 9), (0, 6), (1, 2), (1, 10), (0, 10), (0, 5), (1, 1), (0, 4), (0, 3), (0, 2),
)


def kernel(groups, rows, cols, apart, *refs):
    terms, weights, moments_m, moments_v = (refs[i : i + 3] for i in (0, 3, 6, 9))
    mine_a, mine_b, theirs_a, theirs_b = refs[12:16]
    m_a, m_b, v_a, v_b = refs[16:20]
    y_a, y_b, y_c, z_a, z_b, z_c, w_a, w_b = refs[20:28]
    load_sem, pair_send, pair_recv, y_send, y_recv, z_send, z_recv, spread_send, spread_recv = refs[28:37]
    back_send, back_recv, out_send, out_recv, state_sem, free_sem = refs[37:43]

    rep, me = lax.axis_index("rep"), lax.axis_index("dp")
    c = lax.rem(me, 2)
    z = lax.rem(me // 2, Z)
    y = me // (2 * Z)
    far = Z - 1 - z
    partner = me + 1 - 2 * c
    across = me + (1 - 2 * y) * (2 * Z)
    beside = (me + 2, me - 2)
    place = (z, far)

    def send_to(device, src, dst, send_sem, recv_sem):
        return pltpu.make_async_remote_copy(
            src_ref=src, dst_ref=dst, send_sem=send_sem, recv_sem=recv_sem, device_id=(rep, device), device_id_type=MESH
        )

    def f32(x):
        return x.astype(jnp.float32)

    def part(g, ref):
        width = ref.shape[-1] // cols
        h = lax.rem(g, rows * cols)
        return g // (rows * cols), h // cols, pl.ds(pl.multiple_of(lax.rem(h, cols) * width, width), width)

    def z_first(kind):
        return kind in (DOWN, UP)

    def which(kind):
        return pl.ds(0, 2) if kind == PAIR else pl.ds(0, 1) if kind == GATE else 1

    def new_at(g, kind, *at, theirs=False):
        ref = (theirs_b if theirs else mine_b) if kind == DOWN else theirs_a if theirs else mine_a
        layer, h, width = part(g, ref)
        return ref.at[layer, *at, h, :, width] if kind == DOWN else ref.at[which(kind), layer, *at, h, :, width]

    def new_index(g, weight, i, t):
        layer, h, width = part(g, mine_b if weight == 2 else mine_a)
        return (layer, i, t, h, slice(None), width) if weight == 2 else (weight, layer, i, t, h, slice(None), width)

    def acc_at(g, kind, *at):
        return new_at(g, kind, *at, theirs=True)

    def summed(g, weight, i, t):
        here = new_index(g, weight, i, t)
        return f32(theirs_b[here]) + f32(mine_b[here]) if weight == 2 else f32(theirs_a[here]) + f32(mine_a[here])

    def keep(g, weight, i, t, total):
        if weight == 2:
            theirs_b[new_index(g, weight, i, t)] = total.astype(jnp.bfloat16)
        else:
            theirs_a[new_index(g, weight, i, t)] = total.astype(jnp.bfloat16)

    def tell_partner(kind):
        pl.semaphore_signal(free_sem.at[kind % 2 + kind // 3], inc=1, device_id=(rep, partner), device_id_type=MESH)

    def hear_partner(kind):
        pl.semaphore_wait(free_sem.at[kind % 2 + kind // 3], 1)

    def own_load(g, k):
        layer, h, width = part(g, terms[k])
        dst = theirs_b.at[layer, :, :, h, :, width] if k == 2 else theirs_a.at[k, layer, :, :, h, :, width]
        return pltpu.make_async_copy(terms[k].at[layer, :, :, c, h, :, width], dst, load_sem.at[lax.rem(g, 4), k])

    def pair_copy(g, k):
        layer, h, width = part(g, terms[k])
        src = terms[k].at[layer, :, :, 1 - c, h, :, width]
        dst = mine_b.at[layer, :, :, h, :, width] if k == 2 else mine_a.at[k, layer, :, :, h, :, width]
        return send_to(partner, src, dst, pair_send.at[lax.rem(g, 4), k], pair_recv.at[lax.rem(g, SLOTS), k])

    def slot_of(g, kind):
        if kind == DOWN:
            return lax.rem(g, DOWN_SLOTS)
        return lax.rem(sum(jnp.where(g > one, 1, 0) for one in apart), 2) if kind == UP else lax.rem(g, UP_SLOTS)

    def y_copy(g, kind):
        slot = lax.rem(g, SLOTS)
        if z_first(kind):
            src, dst = acc_at(g, kind, 1 - y, z), (y_b if kind == DOWN else y_c).at[slot_of(g, kind)]
        else:
            src, dst = acc_at(g, kind, 1 - y, slice(None)), y_a.at[lax.rem(g, Y_SLOTS), which(kind)]
        i = kind % 2 + kind // 3
        return send_to(across, src, dst, y_send.at[lax.rem(g, 2), i], y_recv.at[slot, i])

    def z_slot(g, kind, way, s):
        slot = slot_of(g, kind)
        if kind == DOWN:
            return z_b.at[slot, way, s]
        return z_c.at[slot, way, s] if kind == UP else z_a.at[slot, way, s, which(kind)]

    def z_copy(g, kind, way, s):
        t = Z - 1 - s + z if way == 0 else s - far
        src = acc_at(g, kind, slice(None), t) if z_first(kind) else acc_at(g, kind, y, t)
        i = kind % 2 + kind // 3
        sems = z_send.at[lax.rem(g, 2), i, way, s], z_recv.at[lax.rem(g, SLOTS), i, way, s]
        return send_to(beside[way], src, z_slot(g, kind, way, s), *sems)

    def spread_copy(g, kind, way, s, t):
        ref = new_at(g, kind, slice(None) if z_first(kind) else y, t)
        i = kind % 2 + kind // 3
        sems = spread_send.at[lax.rem(g, 2), i, way, s], spread_recv.at[lax.rem(g, SLOTS), i, way, s]
        return send_to(beside[way], ref, ref, *sems)

    def back_copy(g, kind, i, t=None):
        ref = new_at(g, kind, i, slice(None) if t is None else t)
        at = Z + kind // 3 if z_first(kind) else Z + 2 if t is None else t
        return send_to(across, ref, ref, back_send.at[lax.rem(g, 2), at], back_recv.at[lax.rem(g, SLOTS), at])

    def out_copy(g, kind, half):
        at = slice(None) if z_first(kind) else 1 - y if half else y
        i = 2 + kind // 3 if z_first(kind) else half
        src, dst = new_at(g, kind, at, slice(None)), new_at(g, kind, at, slice(None), theirs=True)
        return send_to(partner, src, dst, out_send.at[lax.rem(g, 2), i], out_recv.at[lax.rem(g, SLOTS), i])

    def staged(g, k):
        slot = lax.rem(g, STAGED)
        layer, h, width = part(g, moments_m[k])
        at = (layer, h, slice(None), width) if k == 2 else (k, layer, h, slice(None), width)
        return (w_b.at[slot], m_b.at[at], v_b.at[at]) if k == 2 else (w_a.at[slot, k], m_a.at[at], v_a.at[at])

    def state_loads(g, some):
        slot, copies = lax.rem(g, STAGED), []
        for k in some:
            layer, h, width = part(g, weights[k])
            w_ref, m_ref, v_ref = staged(g, k)
            copies.append(pltpu.make_async_copy(weights[k].at[layer, y, z, c, h, :, width], w_ref, state_sem.at[slot, 3 * k]))
            copies.append(pltpu.make_async_copy(moments_m[k].at[layer, h, :, width], m_ref, state_sem.at[slot, 3 * k + 1]))
            copies.append(pltpu.make_async_copy(moments_v[k].at[layer, h, :, width], v_ref, state_sem.at[slot, 3 * k + 2]))
        return copies

    def z_step(g, kind, s):
        slot = slot_of(g, kind)
        for way in (0, 1):
            t = Z - 1 - s + z if way == 0 else s - far

            def add(arrived, way=way, t=t):
                if z_first(kind):
                    weight = 2 if kind == DOWN else 1
                    came = z_b if kind == DOWN else z_c
                    for i in range(Y):
                        total = summed(g, weight, i, t)
                        if arrived:
                            total += f32(came[slot, way, s - 1, i])
                        keep(g, weight, i, t, total)
                else:
                    for weight in (0, 1) if kind == PAIR else (0,):
                        total = summed(g, weight, y, t) + f32(y_a[lax.rem(g, Y_SLOTS), weight, t])
                        if arrived:
                            total += f32(z_a[slot, way, s - 1, weight])
                        keep(g, weight, y, t, total)
                z_copy(g, kind, way, s).start()

            pl.when(place[way] == 0)(functools.partial(add, False))
            if s:
                pl.when((place[way] >= 1) & (place[way] <= s))(functools.partial(add, True))

    def z_wait(g, kind, s):
        i = kind % 2 + kind // 3
        for way in (0, 1):

            @pl.when((place[way] >= 1) & (place[way] <= s + 1))
            def _(way=way):
                ref = z_slot(g, kind, way, s)
                send_to(beside[way], ref, ref, z_send.at[0, i, way, s], z_recv.at[lax.rem(g, SLOTS), i, way, s]).wait_recv()

            @pl.when((place[way] <= s) & (place[way] < Z - 1))
            def _(way=way):
                z_copy(g, kind, way, s).wait_send()

    def spread_step(g, kind, s):
        for way in (0, 1):

            @pl.when((place[way] >= s) & (place[way] < Z - 1))
            def _(way=way):
                spread_copy(g, kind, way, s, z - s if way == 0 else z + s).start()

    def spread_wait(g, kind, s):
        for way in (0, 1):

            @pl.when(place[way] >= s + 1)
            def _(way=way):
                t = z - 1 - s if way == 0 else z + 1 + s
                spread_copy(g, kind, way, s, t).wait_recv()
                if not z_first(kind):

                    @pl.when(g >= groups - BY_BLOCK)
                    def _():
                        back_copy(g, kind, y, t).start()


            @pl.when((place[way] >= s) & (place[way] < Z - 1))
            def _(way=way):
                spread_copy(g, kind, way, s, z - s if way == 0 else z + s).wait_send()

    def along_z(came, g, kind, *at):
        slot = slot_of(g, kind)
        up, down = f32(came[slot, 0, Z - 2, *at]), f32(came[slot, 1, Z - 2, *at])
        return jnp.where(z >= 1, up, jnp.zeros_like(up)) + jnp.where(far >= 1, down, jnp.zeros_like(down))

    def adamw(g, weight, total):
        w_ref, m_ref, v_ref = staged(g, weight)
        w = f32(w_ref[...])
        gradient = f32(total.astype(jnp.bfloat16))
        m = 0.9 * m_ref[...] + 0.1 * gradient
        v = 0.95 * v_ref[...] + 0.05 * gradient * gradient
        m_ref[...] = m
        v_ref[...] = v
        new = (w - 0.02 * (m * lax.rsqrt(v + 1e-8) + 0.1 * w)).astype(jnp.bfloat16)
        if weight == 2:
            mine_b[new_index(g, weight, y, z)] = new
        else:
            mine_a[new_index(g, weight, y, z)] = new

    def y_first_stage(g, kind, k):
        some = (0, 1) if kind == PAIR else (0,)
        if k == 1:
            for i in some:
                own_load(g, i).wait()
                pair_copy(g, i).wait_recv()
            for i in some:
                for t in range(Z):
                    keep(g, i, 1 - y, t, summed(g, i, 1 - y, t))
            y_copy(g, kind).start()
        if k == 2:
            for i in some:
                pair_copy(g, i).wait_send()
            y_copy(g, kind).wait()
            z_step(g, kind, 0)
        if k in (3, 4):
            z_wait(g, kind, k - 3)
            z_step(g, kind, k - 2)
        if k == 5:
            z_wait(g, kind, 2)
            for i in some:
                adamw(g, i, summed(g, i, y, z) + f32(y_a[lax.rem(g, Y_SLOTS), i, z]) + along_z(z_a, g, kind, i))
            spread_step(g, kind, 0)

            @pl.when(g >= groups - BY_BLOCK)
            def _():
                back_copy(g, kind, y, z).start()

            tell_partner(kind)
        if k in (6, 7):
            spread_wait(g, kind, k - 6)
            spread_step(g, kind, k - 5)
        if k == 8:
            spread_wait(g, kind, 2)

            @pl.when(g < groups - BY_BLOCK)
            def _():
                back_copy(g, kind, y).start()

            hear_partner(kind)
            out_copy(g, kind, 0).start()
        if k == 9:

            @pl.when(g < groups - BY_BLOCK)
            def _():
                back_copy(g, kind, 1 - y).wait_recv()
                back_copy(g, kind, y).wait_send()

            @pl.when(g >= groups - BY_BLOCK)
            def _():
                for t in range(Z):
                    back_copy(g, kind, 1 - y, t).wait_recv()
                    back_copy(g, kind, y, t).wait_send()

            out_copy(g, kind, 1).start()
        if k == 10:
            for half in (0, 1):
                out_copy(g, kind, half).wait()

    def z_first_stage(g, kind, k):
        weight = 2 if kind == DOWN else 1
        came = z_b if kind == DOWN else z_c
        if k == 1:
            own_load(g, weight).wait()
            pair_copy(g, weight).wait_recv()
            z_step(g, kind, 0)
        if k == 2:
            pair_copy(g, weight).wait_send()
        if k in (2, 3):
            z_wait(g, kind, k - 2)
            z_step(g, kind, k - 1)
        if k == 4:
            z_wait(g, kind, 2)
            keep(g, weight, 1 - y, z, summed(g, weight, 1 - y, z) + along_z(came, g, kind, 1 - y))
            y_copy(g, kind).start()
        if k == 5:
            y_copy(g, kind).wait()
            arrived = f32((y_b if kind == DOWN else y_c)[slot_of(g, kind)])
            adamw(g, weight, summed(g, weight, y, z) + arrived + along_z(came, g, kind, y))
            back_copy(g, kind, y, z).start()
            tell_partner(kind)
        if k == 6:
            back_copy(g, kind, 1 - y, z).wait_recv()
            back_copy(g, kind, y, z).wait_send()
            spread_step(g, kind, 0)
        if k in (7, 8):
            spread_wait(g, kind, k - 7)
            spread_step(g, kind, k - 6)
        if k == 9:
            spread_wait(g, kind, 2)
            hear_partner(kind)
            out_copy(g, kind, 0).start()
        if k == 10:
            out_copy(g, kind, 0).wait()

    def is_apart(g):
        found = g < 0
        for one in apart:
            found = found | (g == one)
        return found

    def enter(g):
        for k in range(3):
            pair_copy(g, k).start()
        for k in range(3):
            own_load(g, k).start()

    barrier = pltpu.get_barrier_semaphore()
    for device in (partner, across):
        pl.semaphore_signal(barrier, inc=1, device_id=(rep, device), device_id_type=MESH)
    for way in (0, 1):

        @pl.when(place[way] < Z - 1)
        def _(way=way):
            pl.semaphore_signal(barrier, inc=1, device_id=(rep, beside[way]), device_id_type=MESH)

    pl.semaphore_wait(barrier, 4 - jnp.where(z == 0, 1, 0) - jnp.where(far == 0, 1, 0))

    enter(0)
    enter(1)

    @pl.loop(0, groups + STAGES - 1)
    def _(tick):
        for kind, k in ORDER:
            g = tick - (k - 1)

            @pl.when((g >= 0) & (g < groups))
            def _(g=g, k=k, kind=kind):
                if k == 3 or k == 5:
                    for copy in state_loads(g, (2,) if kind else (0, 1)):
                        if k == 3:
                            copy.start()
                        else:
                            copy.wait()
                if kind == 1:
                    z_first_stage(g, DOWN, k)
                elif apart:
                    here = is_apart(g)

                    @pl.when(jnp.logical_not(here))
                    def _():
                        y_first_stage(g, PAIR, k)

                    @pl.when(here)
                    def _():
                        y_first_stage(g, GATE, k)
                        z_first_stage(g, UP, k)

                else:
                    y_first_stage(g, PAIR, k)

        @pl.when(tick + 2 < groups)
        def _():
            enter(tick + 2)


def put(*refs):
    halves, moments = (refs[0:2], refs[2:4]), (refs[4:6], refs[6:8])
    outs, sem = refs[8:17], refs[17]
    c = lax.rem(lax.axis_index("dp"), 2)
    pairs = []
    for core, (a, b) in zip((c, 1 - c), halves, strict=True):
        for layer in range(b.shape[0]):
            sources = a.at[0, layer], a.at[1, layer], b.at[layer]
            pairs += [(src, out.at[layer, :, :, core]) for src, out in zip(sources, outs[:3], strict=True)]
    for i, (a, b) in enumerate(moments):
        pairs += zip((a.at[0], a.at[1], b), outs[3 + 3 * i : 6 + 3 * i], strict=True)
    copies = [pltpu.make_async_copy(src, dst, sem.at[n]) for n, (src, dst) in enumerate(pairs)]
    for copy in copies:
        copy.start()
    for copy in copies:
        copy.wait()


def in_hbm(x):
    return pltpu.with_memory_space_constraint(x, pltpu.HBM)


def update(terms, weights, m, v, rows=ROWS, cols=COLS, apart=APART):
    layers = weights[0].shape[0]
    groups = layers * rows * cols
    full, own = [], []
    for w in weights:
        lines = w.shape[1] // (2 * Y * Z * rows)
        full.append((layers, Y, Z, 2, rows, lines, w.shape[2]))
        own.append((layers, rows, lines, w.shape[2]))
    halves = (2, *full[0][:3], *full[0][4:]), (*full[2][:3], *full[2][4:])
    a, b = ((s[-2], s[-1] // cols) for s in (full[0], full[2]))
    bf16, dma = jnp.bfloat16, pltpu.SemaphoreType.DMA
    anywhere, vmem = pl.BlockSpec(memory_space=pl.ANY), pl.BlockSpec(memory_space=pltpu.VMEM)
    held = pl.pallas_call(
        functools.partial(kernel, groups, rows, cols, apart),
        out_shape=[pltpu.VMEM(s, bf16) for s in halves] * 2
        + [pltpu.VMEM(s, jnp.float32) for s in ((2, *own[0]), own[2])] * 2,
        in_specs=[anywhere] * 12,
        out_specs=[vmem] * 8,
        scratch_shapes=[
            pltpu.VMEM((Y_SLOTS, 2, Z, *a), bf16),
            pltpu.VMEM((DOWN_SLOTS, *b), bf16),
            pltpu.VMEM((2, *a), bf16),
            pltpu.VMEM((UP_SLOTS, 2, Z - 1, 2, *a), bf16),
            pltpu.VMEM((DOWN_SLOTS, 2, Z - 1, Y, *b), bf16),
            pltpu.VMEM((2, 2, Z - 1, Y, *a), bf16),
            pltpu.VMEM((STAGED, 2, *a), bf16),
            pltpu.VMEM((STAGED, *b), bf16),
            dma((4, 3)),
            dma((4, 3)),
            dma((SLOTS, 3)),
            dma((2, 3)),
            dma((SLOTS, 3)),
            dma((2, 3, 2, Z - 1)),
            dma((SLOTS, 3, 2, Z - 1)),
            dma((2, 3, 2, Z - 1)),
            dma((SLOTS, 3, 2, Z - 1)),
            dma((2, Z + 3)),
            dma((SLOTS, Z + 3)),
            dma((2, 4)),
            dma((SLOTS, 4)),
            dma((STAGED, 9)),
            pltpu.SemaphoreType.REGULAR((3,)),
        ],
        compiler_params=pltpu.CompilerParams(collective_id=0, has_side_effects=True, vmem_limit_bytes=VMEM_BYTES),
        name="sum_step_spread",
    )(
        *[in_hbm(t.reshape(s)) for t, s in zip(terms, full, strict=True)],
        *[in_hbm(w.reshape(s)) for w, s in zip(weights, full, strict=True)],
        *[in_hbm(x.reshape(s)) for x, s in zip(m, own, strict=True)],
        *[in_hbm(x.reshape(s)) for x, s in zip(v, own, strict=True)],
    )
    out = pl.pallas_call(
        put,
        out_shape=[jax.ShapeDtypeStruct(s, bf16) for s in full] + [jax.ShapeDtypeStruct(s, jnp.float32) for s in own] * 2,
        in_specs=[vmem] * 8,
        out_specs=[anywhere] * 9,
        scratch_shapes=[dma((6 + 6 * layers,))],
        compiler_params=pltpu.CompilerParams(vmem_limit_bytes=VMEM_BYTES),
        name="put",
    )(*held)
    return (
        *[o.reshape(w.shape) for o, w in zip(out[:3], weights, strict=True)],
        *[o.reshape(x.shape) for o, x in zip(out[3:6], m, strict=True)],
        *[o.reshape(x.shape) for o, x in zip(out[6:], v, strict=True)],
    )


def solution(mesh):
    def step(*arrays):
        terms, weights, m, v = (arrays[i : i + 3] for i in (0, 3, 6, 9))
        return update([t[0] for t in terms], weights, m, v)

    all_of, cut = P(None, None, None), P(None, "dp", None)
    return jax.shard_map(
        step,
        mesh=mesh,
        in_specs=(P(("rep", "dp"), None, None, None),) * 3 + (all_of,) * 3 + (cut,) * 6,
        out_specs=(P("rep", None, None),) * 3 + (P("rep", "dp", None),) * 6,
        check_vma=False,
    )
```

```python
import functools

import jax
import jax.numpy as jnp
from jax import lax
from jax.experimental import pallas as pl
from jax.experimental.pallas import tpu as pltpu
from jax.sharding import PartitionSpec as P

MESH = pl.DeviceIdType.MESH
Y, Z = 2, 4
ROWS, COLS = 8, 2
SLOTS = 10
Y_SLOTS, UP_SLOTS, DOWN_SLOTS = 9, 5, 7
STAGED = 4
STAGES = 10
BY_BLOCK = 2
PAIR, DOWN, GATE, UP = range(4)
APART = (0, 6, 10, 15, 20)
VMEM_BYTES = 8 * 2**20
ORDER = (
    (1, 7), (1, 5), (1, 6), (1, 4), (0, 8), (0, 7), (1, 3), (1, 9), (1, 8), (0, 1), (0, 9), (0, 6), (1, 2), (1, 10), (0, 10), (0, 5), (1, 1), (0, 4), (0, 3), (0, 2),
)


def kernel(groups, rows, cols, apart, *refs):
    terms, weights, moments_m, moments_v = (refs[i : i + 3] for i in (0, 3, 6, 9))
    mine_a, mine_b, theirs_a, theirs_b = refs[12:16]
    m_a, m_b, v_a, v_b = refs[16:20]
    y_a, y_b, y_c, z_a, z_b, z_c, w_a, w_b = refs[20:28]
    load_sem, pair_send, pair_recv, y_send, y_recv, z_send, z_recv, spread_send, spread_recv = refs[28:37]
    back_send, back_recv, out_send, out_recv, state_sem, free_sem = refs[37:43]

    rep, me = lax.axis_index("rep"), lax.axis_index("dp")
    c = lax.rem(me, 2)
    z = lax.rem(me // 2, Z)
    y = me // (2 * Z)
    far = Z - 1 - z
    partner = me + 1 - 2 * c
    across = me + (1 - 2 * y) * (2 * Z)
    beside = (me + 2, me - 2)
    place = (z, far)

    def send_to(device, src, dst, send_sem, recv_sem):
        return pltpu.make_async_remote_copy(
            src_ref=src, dst_ref=dst, send_sem=send_sem, recv_sem=recv_sem, device_id=(rep, device), device_id_type=MESH
        )

    def f32(x):
        return x.astype(jnp.float32)

    def part(g, ref):
        width = ref.shape[-1] // cols
        h = lax.rem(g, rows * cols)
        return g // (rows * cols), h // cols, pl.ds(pl.multiple_of(lax.rem(h, cols) * width, width), width)

    def z_first(kind):
        return kind in (DOWN, UP)

    def which(kind):
        return pl.ds(0, 2) if kind == PAIR else pl.ds(0, 1) if kind == GATE else 1

    def new_at(g, kind, *at, theirs=False):
        ref = (theirs_b if theirs else mine_b) if kind == DOWN else theirs_a if theirs else mine_a
        layer, h, width = part(g, ref)
        return ref.at[layer, *at, h, :, width] if kind == DOWN else ref.at[which(kind), layer, *at, h, :, width]

    def new_index(g, weight, i, t):
        layer, h, width = part(g, mine_b if weight == 2 else mine_a)
        return (layer, i, t, h, slice(None), width) if weight == 2 else (weight, layer, i, t, h, slice(None), width)

    def acc_at(g, kind, *at):
        return new_at(g, kind, *at, theirs=True)

    def summed(g, weight, i, t):
        here = new_index(g, weight, i, t)
        return f32(theirs_b[here]) + f32(mine_b[here]) if weight == 2 else f32(theirs_a[here]) + f32(mine_a[here])

    def keep(g, weight, i, t, total):
        if weight == 2:
            theirs_b[new_index(g, weight, i, t)] = total.astype(jnp.bfloat16)
        else:
            theirs_a[new_index(g, weight, i, t)] = total.astype(jnp.bfloat16)

    def tell_partner(kind):
        pl.semaphore_signal(free_sem.at[kind % 2 + kind // 3], inc=1, device_id=(rep, partner), device_id_type=MESH)

    def hear_partner(kind):
        pl.semaphore_wait(free_sem.at[kind % 2 + kind // 3], 1)

    def own_load(g, k):
        layer, h, width = part(g, terms[k])
        dst = theirs_b.at[layer, :, :, h, :, width] if k == 2 else theirs_a.at[k, layer, :, :, h, :, width]
        return pltpu.make_async_copy(terms[k].at[layer, :, :, c, h, :, width], dst, load_sem.at[lax.rem(g, 4), k])

    def pair_copy(g, k):
        layer, h, width = part(g, terms[k])
        src = terms[k].at[layer, :, :, 1 - c, h, :, width]
        dst = mine_b.at[layer, :, :, h, :, width] if k == 2 else mine_a.at[k, layer, :, :, h, :, width]
        return send_to(partner, src, dst, pair_send.at[lax.rem(g, 4), k], pair_recv.at[lax.rem(g, SLOTS), k])

    def slot_of(g, kind):
        if kind == DOWN:
            return lax.rem(g, DOWN_SLOTS)
        return lax.rem(sum(jnp.where(g > one, 1, 0) for one in apart), 2) if kind == UP else lax.rem(g, UP_SLOTS)

    def y_copy(g, kind):
        slot = lax.rem(g, SLOTS)
        if z_first(kind):
            src, dst = acc_at(g, kind, 1 - y, z), (y_b if kind == DOWN else y_c).at[slot_of(g, kind)]
        else:
            src, dst = acc_at(g, kind, 1 - y, slice(None)), y_a.at[lax.rem(g, Y_SLOTS), which(kind)]
        i = kind % 2 + kind // 3
        return send_to(across, src, dst, y_send.at[lax.rem(g, 2), i], y_recv.at[slot, i])

    def z_slot(g, kind, way, s):
        slot = slot_of(g, kind)
        if kind == DOWN:
            return z_b.at[slot, way, s]
        return z_c.at[slot, way, s] if kind == UP else z_a.at[slot, way, s, which(kind)]

    def z_copy(g, kind, way, s):
        t = Z - 1 - s + z if way == 0 else s - far
        src = acc_at(g, kind, slice(None), t) if z_first(kind) else acc_at(g, kind, y, t)
        i = kind % 2 + kind // 3
        sems = z_send.at[lax.rem(g, 2), i, way, s], z_recv.at[lax.rem(g, SLOTS), i, way, s]
        return send_to(beside[way], src, z_slot(g, kind, way, s), *sems)

    def spread_copy(g, kind, way, s, t):
        ref = new_at(g, kind, slice(None) if z_first(kind) else y, t)
        i = kind % 2 + kind // 3
        sems = spread_send.at[lax.rem(g, 2), i, way, s], spread_recv.at[lax.rem(g, SLOTS), i, way, s]
        return send_to(beside[way], ref, ref, *sems)

    def back_copy(g, kind, i, t=None):
        ref = new_at(g, kind, i, slice(None) if t is None else t)
        at = Z + kind // 3 if z_first(kind) else Z + 2 if t is None else t
        return send_to(across, ref, ref, back_send.at[lax.rem(g, 2), at], back_recv.at[lax.rem(g, SLOTS), at])

    def out_copy(g, kind, half):
        at = slice(None) if z_first(kind) else 1 - y if half else y
        i = 2 + kind // 3 if z_first(kind) else half
        src, dst = new_at(g, kind, at, slice(None)), new_at(g, kind, at, slice(None), theirs=True)
        return send_to(partner, src, dst, out_send.at[lax.rem(g, 2), i], out_recv.at[lax.rem(g, SLOTS), i])

    def staged(g, k):
        slot = lax.rem(g, STAGED)
        layer, h, width = part(g, moments_m[k])
        at = (layer, h, slice(None), width) if k == 2 else (k, layer, h, slice(None), width)
        return (w_b.at[slot], m_b.at[at], v_b.at[at]) if k == 2 else (w_a.at[slot, k], m_a.at[at], v_a.at[at])

    def state_loads(g, some):
        slot, copies = lax.rem(g, STAGED), []
        for k in some:
            layer, h, width = part(g, weights[k])
            w_ref, m_ref, v_ref = staged(g, k)
            copies.append(pltpu.make_async_copy(weights[k].at[layer, y, z, c, h, :, width], w_ref, state_sem.at[slot, 3 * k]))
            copies.append(pltpu.make_async_copy(moments_m[k].at[layer, h, :, width], m_ref, state_sem.at[slot, 3 * k + 1]))
            copies.append(pltpu.make_async_copy(moments_v[k].at[layer, h, :, width], v_ref, state_sem.at[slot, 3 * k + 2]))
        return copies

    def z_step(g, kind, s):
        slot = slot_of(g, kind)
        for way in (0, 1):
            t = Z - 1 - s + z if way == 0 else s - far

            def add(arrived, way=way, t=t):
                if z_first(kind):
                    weight = 2 if kind == DOWN else 1
                    came = z_b if kind == DOWN else z_c
                    for i in range(Y):
                        total = summed(g, weight, i, t)
                        if arrived:
                            total += f32(came[slot, way, s - 1, i])
                        keep(g, weight, i, t, total)
                else:
                    for weight in (0, 1) if kind == PAIR else (0,):
                        total = summed(g, weight, y, t) + f32(y_a[lax.rem(g, Y_SLOTS), weight, t])
                        if arrived:
                            total += f32(z_a[slot, way, s - 1, weight])
                        keep(g, weight, y, t, total)
                z_copy(g, kind, way, s).start()

            pl.when(place[way] == 0)(functools.partial(add, False))
            if s:
                pl.when((place[way] >= 1) & (place[way] <= s))(functools.partial(add, True))

    def z_wait(g, kind, s):
        i = kind % 2 + kind // 3
        for way in (0, 1):

            @pl.when((place[way] >= 1) & (place[way] <= s + 1))
            def _(way=way):
                ref = z_slot(g, kind, way, s)
                send_to(beside[way], ref, ref, z_send.at[0, i, way, s], z_recv.at[lax.rem(g, SLOTS), i, way, s]).wait_recv()

            @pl.when((place[way] <= s) & (place[way] < Z - 1))
            def _(way=way):
                z_copy(g, kind, way, s).wait_send()

    def spread_step(g, kind, s):
        for way in (0, 1):

            @pl.when((place[way] >= s) & (place[way] < Z - 1))
            def _(way=way):
                spread_copy(g, kind, way, s, z - s if way == 0 else z + s).start()

    def spread_wait(g, kind, s):
        for way in (0, 1):

            @pl.when(place[way] >= s + 1)
            def _(way=way):
                t = z - 1 - s if way == 0 else z + 1 + s
                spread_copy(g, kind, way, s, t).wait_recv()
                if not z_first(kind):

                    @pl.when(g >= groups - BY_BLOCK)
                    def _():
                        back_copy(g, kind, y, t).start()


            @pl.when((place[way] >= s) & (place[way] < Z - 1))
            def _(way=way):
                spread_copy(g, kind, way, s, z - s if way == 0 else z + s).wait_send()

    def along_z(came, g, kind, *at):
        slot = slot_of(g, kind)
        up, down = f32(came[slot, 0, Z - 2, *at]), f32(came[slot, 1, Z - 2, *at])
        return jnp.where(z >= 1, up, jnp.zeros_like(up)) + jnp.where(far >= 1, down, jnp.zeros_like(down))

    def adamw(g, weight, total):
        w_ref, m_ref, v_ref = staged(g, weight)
        w = f32(w_ref[...])
        gradient = f32(total.astype(jnp.bfloat16))
        m = 0.9 * m_ref[...] + 0.1 * gradient
        v = 0.95 * v_ref[...] + 0.05 * gradient * gradient
        m_ref[...] = m
        v_ref[...] = v
        new = (w - 0.02 * (m * lax.rsqrt(v + 1e-8) + 0.1 * w)).astype(jnp.bfloat16)
        if weight == 2:
            mine_b[new_index(g, weight, y, z)] = new
        else:
            mine_a[new_index(g, weight, y, z)] = new

    def y_first_stage(g, kind, k):
        some = (0, 1) if kind == PAIR else (0,)
        if k == 1:
            for i in some:
                own_load(g, i).wait()
                pair_copy(g, i).wait_recv()
            for i in some:
                for t in range(Z):
                    keep(g, i, 1 - y, t, summed(g, i, 1 - y, t))
            y_copy(g, kind).start()
        if k == 2:
            for i in some:
                pair_copy(g, i).wait_send()
            y_copy(g, kind).wait()
            z_step(g, kind, 0)
        if k in (3, 4):
            z_wait(g, kind, k - 3)
            z_step(g, kind, k - 2)
        if k == 5:
            z_wait(g, kind, 2)
            for i in some:
                adamw(g, i, summed(g, i, y, z) + f32(y_a[lax.rem(g, Y_SLOTS), i, z]) + along_z(z_a, g, kind, i))
            spread_step(g, kind, 0)

            @pl.when(g >= groups - BY_BLOCK)
            def _():
                back_copy(g, kind, y, z).start()

            tell_partner(kind)
        if k in (6, 7):
            spread_wait(g, kind, k - 6)
            spread_step(g, kind, k - 5)
        if k == 8:
            spread_wait(g, kind, 2)

            @pl.when(g < groups - BY_BLOCK)
            def _():
                back_copy(g, kind, y).start()

            hear_partner(kind)
            out_copy(g, kind, 0).start()
        if k == 9:

            @pl.when(g < groups - BY_BLOCK)
            def _():
                back_copy(g, kind, 1 - y).wait_recv()
                back_copy(g, kind, y).wait_send()

            @pl.when(g >= groups - BY_BLOCK)
            def _():
                for t in range(Z):
                    back_copy(g, kind, 1 - y, t).wait_recv()
                    back_copy(g, kind, y, t).wait_send()

            out_copy(g, kind, 1).start()
        if k == 10:
            for half in (0, 1):
                out_copy(g, kind, half).wait()

    def z_first_stage(g, kind, k):
        weight = 2 if kind == DOWN else 1
        came = z_b if kind == DOWN else z_c
        if k == 1:
            own_load(g, weight).wait()
            pair_copy(g, weight).wait_recv()
            z_step(g, kind, 0)
        if k == 2:
            pair_copy(g, weight).wait_send()
        if k in (2, 3):
            z_wait(g, kind, k - 2)
            z_step(g, kind, k - 1)
        if k == 4:
            z_wait(g, kind, 2)
            keep(g, weight, 1 - y, z, summed(g, weight, 1 - y, z) + along_z(came, g, kind, 1 - y))
            y_copy(g, kind).start()
        if k == 5:
            y_copy(g, kind).wait()
            arrived = f32((y_b if kind == DOWN else y_c)[slot_of(g, kind)])
            adamw(g, weight, summed(g, weight, y, z) + arrived + along_z(came, g, kind, y))
            back_copy(g, kind, y, z).start()
            tell_partner(kind)
        if k == 6:
            back_copy(g, kind, 1 - y, z).wait_recv()
            back_copy(g, kind, y, z).wait_send()
            spread_step(g, kind, 0)
        if k in (7, 8):
            spread_wait(g, kind, k - 7)
            spread_step(g, kind, k - 6)
        if k == 9:
            spread_wait(g, kind, 2)
            hear_partner(kind)
            out_copy(g, kind, 0).start()
        if k == 10:
            out_copy(g, kind, 0).wait()

    def is_apart(g):
        found = g < 0
        for one in apart:
            found = found | (g == one)
        return found

    def enter(g):
        for k in range(3):
            pair_copy(g, k).start()
        for k in range(3):
            own_load(g, k).start()

    for g in (0, 1):
        for k in range(3):
            own_load(g, k).start()

    barrier = pltpu.get_barrier_semaphore()
    for device in (partner, across):
        pl.semaphore_signal(barrier, inc=1, device_id=(rep, device), device_id_type=MESH)
    for way in (0, 1):

        @pl.when(place[way] < Z - 1)
        def _(way=way):
            pl.semaphore_signal(barrier, inc=1, device_id=(rep, beside[way]), device_id_type=MESH)

    pl.semaphore_wait(barrier, 4 - jnp.where(z == 0, 1, 0) - jnp.where(far == 0, 1, 0))

    for g in (0, 1):
        for k in range(3):
            pair_copy(g, k).start()

    @pl.loop(0, groups + STAGES - 1)
    def _(tick):
        for kind, k in ORDER:
            g = tick - (k - 1)

            @pl.when((g >= 0) & (g < groups))
            def _(g=g, k=k, kind=kind):
                if k == 3 or k == 5:
                    for copy in state_loads(g, (2,) if kind else (0, 1)):
                        if k == 3:
                            copy.start()
                        else:
                            copy.wait()
                if kind == 1:
                    z_first_stage(g, DOWN, k)
                elif apart:
                    here = is_apart(g)

                    @pl.when(jnp.logical_not(here))
                    def _():
                        y_first_stage(g, PAIR, k)

                    @pl.when(here)
                    def _():
                        y_first_stage(g, GATE, k)
                        z_first_stage(g, UP, k)

                else:
                    y_first_stage(g, PAIR, k)

        @pl.when(tick + 2 < groups)
        def _():
            enter(tick + 2)


def put(*refs):
    halves, moments = (refs[0:2], refs[2:4]), (refs[4:6], refs[6:8])
    outs, sem = refs[8:17], refs[17]
    c = lax.rem(lax.axis_index("dp"), 2)
    pairs = []
    for core, (a, b) in zip((c, 1 - c), halves, strict=True):
        for layer in range(b.shape[0]):
            sources = a.at[0, layer], a.at[1, layer], b.at[layer]
            pairs += [(src, out.at[layer, :, :, core]) for src, out in zip(sources, outs[:3], strict=True)]
    for i, (a, b) in enumerate(moments):
        pairs += zip((a.at[0], a.at[1], b), outs[3 + 3 * i : 6 + 3 * i], strict=True)
    copies = [pltpu.make_async_copy(src, dst, sem.at[n]) for n, (src, dst) in enumerate(pairs)]
    for copy in copies:
        copy.start()
    for copy in copies:
        copy.wait()


def in_hbm(x):
    return pltpu.with_memory_space_constraint(x, pltpu.HBM)


def update(terms, weights, m, v, rows=ROWS, cols=COLS, apart=APART):
    layers = weights[0].shape[0]
    groups = layers * rows * cols
    full, own = [], []
    for w in weights:
        lines = w.shape[1] // (2 * Y * Z * rows)
        full.append((layers, Y, Z, 2, rows, lines, w.shape[2]))
        own.append((layers, rows, lines, w.shape[2]))
    halves = (2, *full[0][:3], *full[0][4:]), (*full[2][:3], *full[2][4:])
    a, b = ((s[-2], s[-1] // cols) for s in (full[0], full[2]))
    bf16, dma = jnp.bfloat16, pltpu.SemaphoreType.DMA
    anywhere, vmem = pl.BlockSpec(memory_space=pl.ANY), pl.BlockSpec(memory_space=pltpu.VMEM)
    held = pl.pallas_call(
        functools.partial(kernel, groups, rows, cols, apart),
        out_shape=[pltpu.VMEM(s, bf16) for s in halves] * 2
        + [pltpu.VMEM(s, jnp.float32) for s in ((2, *own[0]), own[2])] * 2,
        in_specs=[anywhere] * 12,
        out_specs=[vmem] * 8,
        scratch_shapes=[
            pltpu.VMEM((Y_SLOTS, 2, Z, *a), bf16),
            pltpu.VMEM((DOWN_SLOTS, *b), bf16),
            pltpu.VMEM((2, *a), bf16),
            pltpu.VMEM((UP_SLOTS, 2, Z - 1, 2, *a), bf16),
            pltpu.VMEM((DOWN_SLOTS, 2, Z - 1, Y, *b), bf16),
            pltpu.VMEM((2, 2, Z - 1, Y, *a), bf16),
            pltpu.VMEM((STAGED, 2, *a), bf16),
            pltpu.VMEM((STAGED, *b), bf16),
            dma((4, 3)),
            dma((4, 3)),
            dma((SLOTS, 3)),
            dma((2, 3)),
            dma((SLOTS, 3)),
            dma((2, 3, 2, Z - 1)),
            dma((SLOTS, 3, 2, Z - 1)),
            dma((2, 3, 2, Z - 1)),
            dma((SLOTS, 3, 2, Z - 1)),
            dma((2, Z + 3)),
            dma((SLOTS, Z + 3)),
            dma((2, 4)),
            dma((SLOTS, 4)),
            dma((STAGED, 9)),
            pltpu.SemaphoreType.REGULAR((3,)),
        ],
        compiler_params=pltpu.CompilerParams(collective_id=0, has_side_effects=True, vmem_limit_bytes=VMEM_BYTES),
        name="sum_step_spread",
    )(
        *[in_hbm(t.reshape(s)) for t, s in zip(terms, full, strict=True)],
        *[in_hbm(w.reshape(s)) for w, s in zip(weights, full, strict=True)],
        *[in_hbm(x.reshape(s)) for x, s in zip(m, own, strict=True)],
        *[in_hbm(x.reshape(s)) for x, s in zip(v, own, strict=True)],
    )
    out = pl.pallas_call(
        put,
        out_shape=[jax.ShapeDtypeStruct(s, bf16) for s in full] + [jax.ShapeDtypeStruct(s, jnp.float32) for s in own] * 2,
        in_specs=[vmem] * 8,
        out_specs=[anywhere] * 9,
        scratch_shapes=[dma((6 + 6 * layers,))],
        compiler_params=pltpu.CompilerParams(vmem_limit_bytes=VMEM_BYTES),
        name="put",
    )(*held)
    return (
        *[o.reshape(w.shape) for o, w in zip(out[:3], weights, strict=True)],
        *[o.reshape(x.shape) for o, x in zip(out[3:6], m, strict=True)],
        *[o.reshape(x.shape) for o, x in zip(out[6:], v, strict=True)],
    )


def solution(mesh):
    def step(*arrays):
        terms, weights, m, v = (arrays[i : i + 3] for i in (0, 3, 6, 9))
        return update([t[0] for t in terms], weights, m, v)

    all_of, cut = P(None, None, None), P(None, "dp", None)
    return jax.shard_map(
        step,
        mesh=mesh,
        in_specs=(P(("rep", "dp"), None, None, None),) * 3 + (all_of,) * 3 + (cut,) * 6,
        out_specs=(P("rep", None, None),) * 3 + (P("rep", "dp", None),) * 6,
        check_vma=False,
    )
```
